256 devices in a mesh: rep: 1, dp: 256 (over x, y, z, core).
Axes of the slice: x: 4, y: 4, z: 8, core: 2. Of those that a mesh axis runs over, the one named last changes fastest.
Arguments:
- x: bfloat16 [256, 1024, 768], P(('rep', 'dp'))
- dy: bfloat16 [256, 1024, 768], P(('rep', 'dp'))
- w_gate: bfloat16 [2, 768, 3072], replicated
- w_up: bfloat16 [2, 768, 3072], replicated
- w_down: bfloat16 [2, 3072, 768], replicated
- m_w_gate: float32 [2, 768, 3072], replicated
- m_w_up: float32 [2, 768, 3072], replicated
- m_w_down: float32 [2, 3072, 768], replicated
- v_w_gate: float32 [2, 768, 3072], replicated
- v_w_up: float32 [2, 768, 3072], replicated
- v_w_down: float32 [2, 3072, 768], replicated
Outputs:
- output 1: bfloat16 [2, 768, 3072], P('rep')
- output 2: bfloat16 [2, 768, 3072], P('rep')
- output 3: bfloat16 [2, 3072, 768], P('rep')
- output 4: float32 [2, 768, 3072], P('rep')
- output 5: float32 [2, 768, 3072], P('rep')
- output 6: float32 [2, 3072, 768], P('rep')
- output 7: float32 [2, 768, 3072], P('rep')
- output 8: float32 [2, 768, 3072], P('rep')
- output 9: float32 [2, 3072, 768], P('rep')
All inputs are finite; a program needn't handle non-finite values.
Results may differ from the reference program's by a relative error of at most 0.022.
Values are sent between devices in bfloat16 or wider.
A program may use at most 768 MiB of HBM per device.

```python
import jax
import jax.numpy as jnp
from jax import lax

SEQUENCES = 256
TOKENS = 1024
D = 768
FF = 3072
LAYERS = 2
NAMES = ("w_gate", "w_up", "w_down")
SHAPES = {"w_gate": (LAYERS, D, FF), "w_up": (LAYERS, D, FF), "w_down": (LAYERS, FF, D)}


def bump(key, n, height):
    away = (jnp.arange(n, dtype=jnp.int32) - jax.random.randint(key, (), 0, n, jnp.int32)) % n
    return jnp.where(away < n // 8, height, 1.0)


def together(key, own, strength):
    shared = jax.random.normal(key, own.shape[1:], jnp.float32)
    return (own + strength * shared) * lax.rsqrt(1 + strength * strength)


def setup_inputs(seed: int = 0, part: int = 0) -> dict:
    kx, kdy, ka, kb, kz, kf, kh, kl, *keys = jax.random.split(jax.random.key(seed), 8 + 3 * len(NAMES))
    kx, kdy, ka, kb = (jax.random.fold_in(k, part) for k in (kx, kdy, ka, kb))
    kw, km, kv = (keys[i::3] for i in range(3))
    shape = (SEQUENCES, TOKENS, D)
    much_x, much_dy = jax.random.uniform(kz, (2,), jnp.float32, 0.0, 1.0)
    loud = 2.0 ** jax.random.uniform(jax.random.fold_in(kz, 1), (), jnp.float32, -1.0, 2.0)
    layers = 2.0 ** jax.random.uniform(kl, (LAYERS, 1, 1), jnp.float32, -1.0, 1.0)
    x = together(ka, jax.random.normal(kx, shape, jnp.float32), much_x) * bump(kf, D, 4.0)
    dy = together(kb, jax.random.normal(kdy, shape, jnp.float32), much_dy)
    drawn = {"x": x.astype(jnp.bfloat16), "dy": (loud * dy * (SEQUENCES * TOKENS) ** -0.5).astype(jnp.bfloat16)}
    for key, name in zip(kw, NAMES, strict=True):
        w = jax.random.normal(key, SHAPES[name], jnp.float32) * SHAPES[name][1] ** -0.5
        drawn[name] = (w * {"w_gate": 1.0, "w_up": bump(kh, FF, 4.0), "w_down": layers}[name]).astype(jnp.bfloat16)
    for key, name in zip(km, NAMES, strict=True):
        drawn[f"m_{name}"] = 0.1 * jax.random.normal(key, SHAPES[name], jnp.float32)
    for key, name in zip(kv, NAMES, strict=True):
        drawn[f"v_{name}"] = loud * loud * jax.random.uniform(key, SHAPES[name], jnp.float32, 0.05, 0.15)
    return drawn


def matmul(a, w):
    return jnp.dot(a, w, preferred_element_type=jnp.float32).astype(jnp.bfloat16)


def normed(h):
    wide = h.astype(jnp.float32)
    scale = lax.rsqrt(jnp.mean(wide**2, -1, keepdims=True) + 1e-6)
    return (wide * scale).astype(jnp.bfloat16)


def layer(h, w):
    a = normed(h)
    gate = jnp.dot(a, w["w_gate"], preferred_element_type=jnp.float32)
    up = jnp.dot(a, w["w_up"], preferred_element_type=jnp.float32)
    return h + matmul((jax.nn.silu(gate) * up).astype(jnp.bfloat16), w["w_down"])


def adamw(w, m, v, g):
    m = 0.9 * m + 0.1 * g
    v = 0.95 * v + 0.05 * g * g
    step = m * lax.rsqrt(v + 1e-8) + 0.1 * w
    return (w - 0.02 * step).astype(jnp.bfloat16), m, v


def stack(weights, h):
    return lax.scan(lambda h, w: (layer(h, w), None), h, weights)[0]


def reference(x, dy, w_gate, w_up, w_down, m_w_gate, m_w_up, m_w_down, v_w_gate, v_w_up, v_w_down):
    weights = dict(zip(NAMES, (w_gate, w_up, w_down), strict=True))

    def take(so_far, sequence):
        h, by_y = sequence
        _, back = jax.vjp(lambda w: stack(w, h), weights)
        return jax.tree.map(lambda total, term: total + term.astype(jnp.float32), so_far, back(by_y)[0]), None

    none_yet = {name: jnp.zeros(w.shape, jnp.float32) for name, w in weights.items()}
    by_weights, _ = lax.scan(take, none_yet, (x, dy))
    gradients = [by_weights[name].astype(jnp.bfloat16).astype(jnp.float32) for name in NAMES]
    new = [
        adamw(w.astype(jnp.float32), m, v, g)
        for w, m, v, g in zip((w_gate, w_up, w_down), (m_w_gate, m_w_up, m_w_down), (v_w_gate, v_w_up, v_w_down), gradients, strict=True)
    ]
    return tuple(one[which] for which in range(3) for one in new)
```

```python
import functools

import jax
import jax.numpy as jnp
from jax import lax
from jax.experimental import pallas as pl
from jax.experimental.pallas import tpu as pltpu
from jax.sharding import PartitionSpec as P

NAMES = ("w_gate", "w_up", "w_down")
MESH = pl.DeviceIdType.MESH
F32, BF16 = jnp.float32, jnp.bfloat16
LANES = 128

def chunk_of(n, cap=128):
    best = 16
    for c in range(16, cap + 1, 16):
        if n % c == 0:
            best = c
    return best

def over_rows(n, body, cap=128):
    c = chunk_of(n, cap)
    if n == c:
        body(0, c)
    else:
        def step(i, _):
            body(pl.multiple_of(i * c, 16), c)
            return 0
        lax.fori_loop(0, n // c, step, 0)

class Color:
    def __init__(self, name, off, S, dims, n):
        self.name, self.off, self.S, self.dims = name, off, S, dims
        self.n1, self.n2, self.n3 = (n[d] for d in dims)
        self.L = S // self.n1
        self.La = (self.L // 2) // 16 * 16
        self.Lb = self.L - self.La
        self.L2 = self.L // self.n2
        self.La2 = (self.L2 // 2) // 16 * 16
        self.Lb2 = self.L2 - self.La2
        assert S % (self.n1 * self.n2 * 16) == 0 and self.Lb % self.L2 == 0 and self.La2 > 0, (S, self.L, self.L2)
        h1, h2 = self.n1 // 2, self.n2 // 2
        self.h1, self.h2 = h1, h2
        self.m_rs1, self.m_rs2 = 0, 2 * h1
        self.m_y = self.m_rs2 + 2 * h2
        self.m_ag2 = self.m_y + self.n3 - 1
        self.m_ag1 = self.m_ag2 + 2 * h2
        self.m_pair = self.m_ag1 + 2 * h1
        self.nmsg = self.m_pair + 1
    def scratch(self, NB):
        return [pltpu.VMEM((NB, (self.n1 - 1) * self.L, LANES), BF16),
                pltpu.VMEM((NB, self.L, LANES), F32),
                pltpu.VMEM((NB, self.L, LANES), BF16),
                pltpu.VMEM((NB, (self.n2 - 1) * self.L2, LANES), BF16),
                pltpu.VMEM((NB, self.L2, LANES), F32),
                pltpu.VMEM((NB, self.n3, self.L2, LANES), BF16),
                pltpu.SemaphoreType.DMA((NB, self.nmsg)), pltpu.SemaphoreType.DMA((NB, self.nmsg))]

def m16(v):
    return pl.multiple_of(v, 16)

class Comm:
    def __init__(self, n, cfg, B, NB):
        self.n, self.B, self.NB = n, B, NB
        off, self.colors = 0, []
        for name, rows, dims in cfg:
            self.colors.append(Color(name, off, rows, dims, n)); off += rows
        self.HB, self.TB = off, 2 * off
    def scratch(self):
        out = [pltpu.VMEM((self.B, self.TB, LANES), BF16), pltpu.VMEM((self.NB, self.HB, LANES), BF16),
               pltpu.SemaphoreType.DMA((self.NB,)), pltpu.SemaphoreType.DMA((self.NB,))]
        for c in self.colors:
            out += c.scratch(self.NB)
        return out
    def setup(self, scratch):
        n = self.n
        me = lax.axis_index("dp")
        core = lax.rem(me, 2); z = lax.rem(lax.div(me, 2), n["z"])
        y = lax.rem(lax.div(me, 2 * n["z"]), n["y"]); x = lax.div(me, 2 * n["z"] * n["y"])
        self.pos = {"x": x, "y": y, "z": z}
        self.core = core
        stride = {"x": 2 * n["z"] * n["y"], "y": 2 * n["z"], "z": 2}
        def shifted(d, k):
            q = lax.rem(self.pos[d] + k + n[d], n[d])
            return me + (q - self.pos[d]) * stride[d]
        self.shifted = shifted
        self.partner = me + 1 - 2 * core
        self.G, self.D, self.ds, self.dr = scratch[:4]
        self.bufs = {}
        rest = scratch[4:]
        for i, c in enumerate(self.colors):
            self.bufs[c.name] = rest[8 * i:8 * i + 8]
        self.mine = core * self.HB
        self.other = (1 - core) * self.HB
    def barrier(self):
        n = self.n
        peers = [self.partner]
        need = {d: set() for d in "xyz"}
        for c in self.colors:
            for d in c.dims[:2]:
                need[d] |= {1 % n[d], (n[d] - 1) % n[d]}
            need[c.dims[2]] |= set(range(1, n[c.dims[2]]))
        for d in "xyz":
            for k in sorted(need[d]):
                if k:
                    peers.append(self.shifted(d, k))
        sem = pltpu.get_barrier_semaphore()
        for p in peers:
            pl.semaphore_signal(sem, inc=1, device_id={"dp": p}, device_id_type=MESH)
        pl.semaphore_wait(sem, len(peers))
    def copy(self, src, dst, ss, rs, dev):
        return pltpu.make_async_remote_copy(src_ref=src, dst_ref=dst, send_sem=ss, recv_sem=rs, device_id={"dp": dev}, device_id_type=MESH)

    def pair_copy(self, b):
        s = lax.rem(b, self.NB)
        return self.copy(self.G.at[b, pl.ds(m16(self.other), self.HB)], self.D.at[s], self.ds.at[s], self.dr.at[s], self.partner)
    def phases(self):
        out = [[lambda b: self.pair_copy(b).start()], [lambda b: self.pair_copy(b).wait()]]
        per = [self.color_phases(c) for c in self.colors]
        depth = max(len(p) for p in per)
        out += [[] for _ in range(depth - 1)]
        for p in per:
            for i, f in enumerate(p):
                out[1 + i].append(f)
        return out

    def color_phases(self, c):
        G, D = self.G, self.D
        R1, O1, O1b, R2, O2, Y, SS, RS = self.bufs[c.name]
        NB = self.NB
        p1, p2, p3 = (self.pos[d] for d in c.dims)
        r1, l1 = self.shifted(c.dims[0], 1), self.shifted(c.dims[0], -1)
        r2, l2 = self.shifted(c.dims[1], 1), self.shifted(c.dims[1], -1)
        n1, n2, n3, h1, h2 = c.n1, c.n2, c.n3, c.h1, c.h2
        L, La, Lb, L2, La2, Lb2 = c.L, c.La, c.Lb, c.L2, c.La2, c.Lb2
        mod = lambda v, n: lax.rem(v + 4 * n, n)
        base = self.mine + c.off
        dbase = c.off
        sl = lambda b: lax.rem(b, NB)

        def ring(stage):
            if stage == 1:
                return dict(n=n1, h=h1, L=L, La=La, Lb=Lb, p=p1, right=r1, left=l1, R=R1, m=c.m_rs1)
            return dict(n=n2, h=h2, L=L2, La=La2, Lb=Lb2, p=p2, right=r2, left=l2, R=R2, m=c.m_rs2)
        def local(stage, b, row, k):
            if stage == 1:
                return G[b, pl.ds(m16(base + row), k), :].astype(F32) + D[sl(b), pl.ds(m16(dbase + row), k), :].astype(F32)
            return O1[sl(b), pl.ds(m16(row), k), :] + R1[sl(b), pl.ds(m16(2 * (h1 - 1) * L + row), k), :].astype(F32)
        def staged(stage, b, row, k):
            if stage == 1:
                return D.at[sl(b), pl.ds(m16(dbase + row), k)]
            return O1b.at[sl(b), pl.ds(m16(row), k)]
        def rs_copy(stage, b, k, direction):
            g = ring(stage)
            n, h, LL, A, Bb = g["n"], g["h"], g["L"], g["La"], g["Lb"]
            s = sl(b)
            if k < h:
                slot = mod(g["p"] + h - k + 1, n) if direction == 0 else mod(g["p"] - h + k, n)
                src = staged(stage, b, slot * LL, LL)
                dst = g["R"].at[s, pl.ds((k - 1) * 2 * LL + direction * LL, LL)]
            elif direction == 0:
                src = staged(stage, b, mod(g["p"] + 1, n) * LL + A, Bb)
                dst = g["R"].at[s, pl.ds((h - 1) * 2 * LL, Bb)]
            else:
                src = staged(stage, b, g["p"] * LL, A)
                dst = g["R"].at[s, pl.ds((h - 1) * 2 * LL + Bb, A)]
            m = g["m"] + 2 * (k - 1) + direction
            return self.copy(src, dst, SS.at[s, m], RS.at[s, m], g["right"] if direction == 0 else g["left"])
        def rs_step(stage, k):
            def f(b):
                g = ring(stage)
                n, h, LL, A, Bb = g["n"], g["h"], g["L"], g["La"], g["Lb"]
                s = sl(b)
                for direction in (0, 1):
                    if k > 1:
                        rs_copy(stage, b, k - 1, direction).wait()
                    slot = mod(g["p"] + h - k + 1, n) if direction == 0 else mod(g["p"] - h + k, n)
                    rin = (k - 2) * 2 * LL + direction * LL
                    def total(row, at, kk):
                        v = local(stage, b, row, kk)
                        if k > 1:
                            v = v + g["R"][s, pl.ds(m16(rin + at), kk), :].astype(F32)
                        return v
                    def send_part(lo, cnt):
                        def body(i, kk):
                            v = total(slot * LL + lo + i, lo + i, kk)
                            ref = D if stage == 1 else O1b
                            o = (dbase if stage == 1 else 0) + slot * LL + lo + i
                            ref[s, pl.ds(m16(o), kk), :] = v.astype(BF16)
                        over_rows(cnt, body)
                    def keep_part(lo, cnt, to):
                        ref = O1 if stage == 1 else O2
                        def body(i, kk):
                            ref[s, pl.ds(m16(to + i), kk), :] = total(slot * LL + lo + i, lo + i, kk)
                        over_rows(cnt, body)
                    if k < h:
                        send_part(0, LL)
                        rs_copy(stage, b, k, direction).start()
                    elif direction == 0:
                        send_part(A, Bb)
                        rs_copy(stage, b, k, direction).start()
                        keep_part(0, A, Bb)
                    else:
                        send_part(0, A)
                        rs_copy(stage, b, k, direction).start()
                        keep_part(A, Bb, 0)
            return f
        def rs_end(stage):
            def f(b):
                for direction in (0, 1):
                    rs_copy(stage, b, ring(stage)["h"], direction).wait()
            return f
        def y_copy(b, k):
            s = sl(b)
            m = c.m_y + k - 1
            return self.copy(Y.at[s, p3], Y.at[s, p3], SS.at[s, m], RS.at[s, m], self.shifted(c.dims[2], k))
        def y_wait(b, k):
            s = sl(b)
            m = c.m_y + k - 1
            return self.copy(Y.at[s, p3], Y.at[s, mod(p3 - k, n3)], SS.at[s, m], RS.at[s, m], self.shifted(c.dims[2], k))
        def y_send(b):
            s = sl(b)
            def body(i, kk):
                v = O2[s, pl.ds(i, kk), :] + R2[s, pl.ds(m16(2 * (h2 - 1) * L2 + i), kk), :].astype(F32)
                Y[s, p3, pl.ds(i, kk), :] = v.astype(BF16)
            over_rows(L2, body)
            for k in range(1, n3):
                y_copy(b, k).start()
        def grow(v):
            return base + mod(p1 * L + La + v, c.S)
        def y_sum(b):
            s = sl(b)
            for k in range(1, n3):
                y_wait(b, k).wait()
            def part(src, cnt, row):
                def body(i, kk):
                    v = Y[s, 0, pl.ds(m16(src + i), kk), :].astype(F32)
                    for j in range(1, n3):
                        v = v + Y[s, j, pl.ds(m16(src + i), kk), :].astype(F32)
                    G[b, pl.ds(m16(row + i), kk), :] = v.astype(BF16)
                over_rows(cnt, body)
            part(0, Lb2, grow(p2 * L2 + La2))
            part(Lb2, La2, grow(mod(p2 + 1, n2) * L2))
        def ag_copy(stage, b, k, direction):
            s = sl(b)
            if stage == 2:
                n, LL, A, Bb, p, right, left, m = n2, L2, La2, Lb2, p2, r2, l2, c.m_ag2
                at = lambda slot, part: grow(slot * L2) + part
            else:
                n, LL, A, Bb, p, right, left, m = n1, L, La, Lb, p1, r1, l1, c.m_ag1
                at = lambda slot, part: base + slot * L + part
            if k == 1:
                row, cnt = (at(mod(p + 1, n), 0), A) if direction == 0 else (at(p, A), Bb)
            else:
                row, cnt = (at(mod(p - (k - 2), n), 0) if direction == 0 else at(mod(p + 1 + (k - 2), n), 0)), LL
            ref = G.at[b, pl.ds(m16(row), cnt)]
            mm = m + 2 * (k - 1) + direction
            return self.copy(ref, ref, SS.at[s, mm], RS.at[s, mm], right if direction == 0 else left)
        def ag_in(stage, b, k, direction):
            s = sl(b)
            if stage == 2:
                n, LL, A, Bb, p, right, left, m = n2, L2, La2, Lb2, p2, r2, l2, c.m_ag2
                at = lambda slot, part: grow(slot * L2) + part
            else:
                n, LL, A, Bb, p, right, left, m = n1, L, La, Lb, p1, r1, l1, c.m_ag1
                at = lambda slot, part: base + slot * L + part
            if k == 1:
                row, cnt = (at(p, 0), A) if direction == 0 else (at(mod(p + 1, n), A), Bb)
            else:
                row, cnt = (at(mod(p - 1 - (k - 2), n), 0) if direction == 0 else at(mod(p + 2 + (k - 2), n), 0)), LL
            ref = G.at[b, pl.ds(m16(row), cnt)]
            mm = m + 2 * (k - 1) + direction
            return self.copy(ref, ref, SS.at[s, mm], RS.at[s, mm], right if direction == 0 else left)
        def ag_wait(stage, b, k):
            for direction in (0, 1):
                ag_copy(stage, b, k, direction).wait_send()
                ag_in(stage, b, k, direction).wait_recv()
        def ag_start(stage, b, k):
            for direction in (0, 1):
                ag_copy(stage, b, k, direction).start()
        def pair(b):
            s = sl(b)
            ref = G.at[b, pl.ds(m16(base), c.S)]
            return self.copy(ref, ref, SS.at[s, c.m_pair], RS.at[s, c.m_pair], self.partner)
        def pair_in(b):
            s = sl(b)
            ref = G.at[b, pl.ds(m16(self.other + c.off), c.S)]
            return self.copy(ref, ref, SS.at[s, c.m_pair], RS.at[s, c.m_pair], self.partner)

        out = []
        for k in range(1, h1 + 1):
            out.append(rs_step(1, k))
        for k in range(1, h2 + 1):
            if k == 1:
                out.append(lambda b: (rs_end(1)(b), rs_step(2, 1)(b)))
            else:
                out.append(rs_step(2, k))
        out.append(lambda b: (rs_end(2)(b), y_send(b)))
        out.append(lambda b: (y_sum(b), ag_start(2, b, 1)))
        for k in range(2, h2 + 1):
            out.append(lambda b, k=k: (ag_wait(2, b, k - 1), ag_start(2, b, k)))
        out.append(lambda b: (ag_wait(2, b, h2), ag_start(1, b, 1)))
        for k in range(2, h1 + 1):
            out.append(lambda b, k=k: (ag_wait(1, b, k - 1), ag_start(1, b, k)))
        out.append(lambda b: (ag_wait(1, b, h1), pair(b).start()))
        out.append(lambda b: (pair(b).wait_send(), pair_in(b).wait_recv()))
        return out

def kernel(comm, K, g_hbm, o_hbm, *scratch):
    B = comm.B
    cs, lsem, osem = scratch[:-2], scratch[-2], scratch[-1]
    comm.setup(cs)
    load = lambda b: pltpu.make_async_copy(g_hbm.at[b], comm.G.at[b], lsem.at[b])
    store = lambda b: pltpu.make_async_copy(comm.G.at[b], o_hbm.at[b], osem.at[b])
    for b in range(B):
        load(b).start()
    comm.barrier()
    phases = comm.phases()
    nph = len(phases)
    depth = -(-nph // K)
    def iteration(it, _):
        for sub in range(K):
            for i in range(depth):
                ph = sub + K * i
                if ph >= nph:
                    continue
                b = it - i
                @pl.when((b >= 0) & (b < B))
                def _():
                    if ph == 0:
                        load(b).wait()
                    for f in phases[ph]:
                        f(b)
                    if ph == nph - 1:
                        store(b).start()
        return 0
    lax.fori_loop(0, B + depth - 1, iteration, 0)
    def fin(b, _):
        store(b).wait()
        return 0
    lax.fori_loop(0, B, fin, 0)

def allsum(comm, K, g, vmem=66_000_000):
    return pl.pallas_call(
        functools.partial(kernel, comm, K),
        out_shape=jax.ShapeDtypeStruct((comm.B, comm.TB, LANES), BF16),
        in_specs=[pl.BlockSpec(memory_space=pl.ANY)], out_specs=pl.BlockSpec(memory_space=pl.ANY),
        scratch_shapes=comm.scratch() + [pltpu.SemaphoreType.DMA((comm.B,)), pltpu.SemaphoreType.DMA((comm.B,))],
        compiler_params=pltpu.CompilerParams(collective_id=0, has_side_effects=True, vmem_limit_bytes=vmem),
    )(g)
def matmul(a, w):
    return jnp.dot(a, w, preferred_element_type=jnp.float32).astype(jnp.bfloat16)


def normed(h):
    wide = h.astype(jnp.float32)
    scale = lax.rsqrt(jnp.mean(wide**2, -1, keepdims=True) + 1e-6)
    return (wide * scale).astype(jnp.bfloat16)


def layer(h, w):
    a = normed(h)
    gate = jnp.dot(a, w["w_gate"], preferred_element_type=jnp.float32)
    up = jnp.dot(a, w["w_up"], preferred_element_type=jnp.float32)
    return h + matmul((jax.nn.silu(gate) * up).astype(jnp.bfloat16), w["w_down"])


def adamw(w, m, v, g):
    m = 0.9 * m + 0.1 * g
    v = 0.95 * v + 0.05 * g * g
    step = m * lax.rsqrt(v + 1e-8) + 0.1 * w
    return (w - 0.02 * step).astype(jnp.bfloat16), m, v


TILE = 16
COLORS = (("a", 224 * TILE, "xzy"), ("b", 224 * TILE, "yzx"), ("c", 128 * TILE, "zxy"))
SIZES = {"x": 4, "y": 4, "z": 8}
PARTS = 3


def pack(g, l):
    gate, up, down = g
    d, f = gate.shape
    step = f // PARTS
    cols = lambda t: t.reshape(d, PARTS, step // LANES, LANES).transpose(1, 2, 0, 3).reshape(PARTS, -1, LANES)
    rows = down.reshape(PARTS, step, d // LANES, LANES).transpose(0, 2, 1, 3).reshape(PARTS, -1, LANES)
    return jnp.concatenate([cols(gate), cols(up), rows], 1)


def unpack(s, d, f):
    step = f // PARTS
    n = step * d // LANES
    cols = lambda t: t.reshape(2, PARTS, step // LANES, d, LANES).transpose(0, 3, 1, 2, 4).reshape(2, d, f)
    rows = lambda t: t.reshape(2, PARTS, d // LANES, step, LANES).transpose(0, 1, 3, 2, 4).reshape(2, f, d)
    return cols(s[:, :n]), cols(s[:, n : 2 * n]), rows(s[:, 2 * n :])


def solution(mesh):
    comm = Comm(SIZES, COLORS, 2 * PARTS, 4)

    def step(x, dy, *arrays):
        weights, m, v = (arrays[i : i + 3] for i in (0, 3, 6))
        layers = weights[0].shape[0]
        h, kept = x[0], []
        for number in range(layers):
            kept.append(h)
            h = layer(h, {name: w[number] for name, w in zip(NAMES, weights, strict=True)})
        by_h, terms = dy[0], [None] * layers
        for number in reversed(range(layers)):
            _, back = jax.vjp(lambda w, h: layer(h, w), {name: w[number] for name, w in zip(NAMES, weights, strict=True)}, kept[number])
            by_w, by_h = back(by_h)
            terms[number] = pack([by_w[name] for name in NAMES], number)
        summed = allsum(comm, 4, jnp.concatenate([terms[1], terms[0]], 0))
        summed = jnp.concatenate([summed[PARTS:], summed[:PARTS]], 0)
        d, f = weights[0].shape[1:]
        gradients = [g.astype(jnp.float32) for g in unpack(summed, d, f)]
        new = [adamw(w.astype(jnp.float32), m, v, g) for w, m, v, g in zip(weights, m, v, gradients, strict=True)]
        return tuple(one[which] for which in range(3) for one in new)

    return jax.shard_map(
        step,
        mesh=mesh,
        in_specs=(P(("rep", "dp"), None, None),) * 2 + (P(None, None, None),) * 9,
        out_specs=(P("rep", None, None),) * 9,
        check_vma=False,
    )
```

```python
import functools
import jax
import jax.numpy as jnp
from jax import lax
from jax.experimental import pallas as pl
from jax.experimental.pallas import tpu as pltpu
from jax.sharding import PartitionSpec as P
MESH = pl.DeviceIdType.MESH
F32, BF16 = jnp.float32, jnp.bfloat16
LANES = 128

def chunk_of(n, cap=256):
    best = 16
    for c in range(16, cap + 1, 16):
        if n % c == 0:
            best = c
    return best

def over_rows(n, body, cap=256):
    c = chunk_of(n, cap)
    if n == c:
        body(0, c)
    else:
        def step(i, _):
            body(pl.multiple_of(i * c, 16), c)
            return 0
        lax.fori_loop(0, n // c, step, 0)

class Color:
    def __init__(self, name, off, S, dims, n):
        self.name, self.off, self.S, self.dims = name, off, S, dims
        self.n1, self.n2, self.n3 = (n[d] for d in dims)
        self.L = S // self.n1
        self.La = (self.L // 2) // 16 * 16
        self.Lb = self.L - self.La
        self.L2 = self.L // self.n2
        self.La2 = (self.L2 // 2) // 16 * 16
        self.Lb2 = self.L2 - self.La2
        assert S % (self.n1 * self.n2 * 16) == 0 and self.Lb % self.L2 == 0 and self.La2 > 0, (S, self.L, self.L2)
        h1, h2 = self.n1 // 2, self.n2 // 2
        self.h1, self.h2 = h1, h2
        self.m_rs1, self.m_rs2 = 0, 2 * h1
        self.m_y = self.m_rs2 + 2 * h2
        self.m_ag2 = self.m_y + self.n3 - 1
        self.m_ag1 = self.m_ag2 + 2 * h2
        self.m_pair = self.m_ag1 + 2 * h1
        self.nmsg = self.m_pair + 1
    def scratch(self, NB):
        return [pltpu.VMEM((NB, (self.n1 - 1) * self.L, LANES), BF16),
                pltpu.VMEM((NB, self.L, LANES), F32),
                pltpu.VMEM((NB, self.L, LANES), BF16),
                pltpu.VMEM((NB, (self.n2 - 1) * self.L2, LANES), BF16),
                pltpu.VMEM((NB, self.L2, LANES), F32),
                pltpu.VMEM((NB, self.n3, self.L2, LANES), BF16),
                pltpu.SemaphoreType.DMA((NB, self.nmsg)), pltpu.SemaphoreType.DMA((NB, self.nmsg))]

def m16(v):
    return pl.multiple_of(v, 16)

class Comm:
    def __init__(self, n, cfg, B, NB, ND=None):
        self.n, self.B, self.NB, self.ND = n, B, NB, ND or NB
        off, self.colors = 0, []
        for name, rows, dims in cfg:
            self.colors.append(Color(name, off, rows, dims, n)); off += rows
        self.HB, self.TB = off, 2 * off
    def scratch(self):
        out = [pltpu.VMEM((self.B, self.TB, LANES), BF16), pltpu.VMEM((self.ND, self.HB, LANES), BF16),
               pltpu.SemaphoreType.DMA((self.ND,)), pltpu.SemaphoreType.DMA((self.ND,))]
        for c in self.colors:
            out += c.scratch(self.NB)
        return out
    def setup(self, scratch):
        n = self.n
        me = lax.axis_index("dp")
        core = lax.rem(me, 2); z = lax.rem(lax.div(me, 2), n["z"])
        y = lax.rem(lax.div(me, 2 * n["z"]), n["y"]); x = lax.div(me, 2 * n["z"] * n["y"])
        self.pos = {"x": x, "y": y, "z": z}
        self.core = core
        stride = {"x": 2 * n["z"] * n["y"], "y": 2 * n["z"], "z": 2}
        def shifted(d, k):
            q = lax.rem(self.pos[d] + k + n[d], n[d])
            return me + (q - self.pos[d]) * stride[d]
        self.shifted = shifted
        self.partner = me + 1 - 2 * core
        self.G, self.D, self.ds, self.dr = scratch[:4]
        self.bufs = {}
        rest = scratch[4:]
        for i, c in enumerate(self.colors):
            self.bufs[c.name] = rest[8 * i:8 * i + 8]
        self.mine = core * self.HB
        self.other = (1 - core) * self.HB
    def barrier(self):
        n = self.n
        peers = [self.partner]
        need = {d: set() for d in "xyz"}
        for c in self.colors:
            for d in c.dims[:2]:
                need[d] |= {1 % n[d], (n[d] - 1) % n[d]}
            need[c.dims[2]] |= set(range(1, n[c.dims[2]]))
        for d in "xyz":
            for k in sorted(need[d]):
                if k:
                    peers.append(self.shifted(d, k))
        sem = pltpu.get_barrier_semaphore()
        for p in peers:
            pl.semaphore_signal(sem, inc=1, device_id={"dp": p}, device_id_type=MESH)
        pl.semaphore_wait(sem, len(peers))
    def copy(self, src, dst, ss, rs, dev):
        return pltpu.make_async_remote_copy(src_ref=src, dst_ref=dst, send_sem=ss, recv_sem=rs, device_id={"dp": dev}, device_id_type=MESH)

    def pair_copy(self, b):
        s = lax.rem(b, self.ND)
        return self.copy(self.G.at[b, pl.ds(m16(self.other), self.HB)], self.D.at[s], self.ds.at[s], self.dr.at[s], self.partner)
    def phases(self):
        out = [[lambda b: self.pair_copy(b).start()], [lambda b: self.pair_copy(b).wait()]]
        per = [self.color_phases(c) for c in self.colors]
        depth = max(len(p) for p in per)
        out += [[] for _ in range(depth - 1)]
        for p in per:
            for i, f in enumerate(p):
                out[1 + i].append(f)
        return out

    def color_phases(self, c):
        G, D = self.G, self.D
        R1, O1, O1b, R2, O2, Y, SS, RS = self.bufs[c.name]
        NB = self.NB
        p1, p2, p3 = (self.pos[d] for d in c.dims)
        r1, l1 = self.shifted(c.dims[0], 1), self.shifted(c.dims[0], -1)
        r2, l2 = self.shifted(c.dims[1], 1), self.shifted(c.dims[1], -1)
        n1, n2, n3, h1, h2 = c.n1, c.n2, c.n3, c.h1, c.h2
        L, La, Lb, L2, La2, Lb2 = c.L, c.La, c.Lb, c.L2, c.La2, c.Lb2
        mod = lambda v, n: lax.rem(v + 4 * n, n)
        base = self.mine + c.off
        dbase = c.off
        sl = lambda b: lax.rem(b, NB)
        dsl = lambda b: lax.rem(b, self.ND)

        def ring(stage):
            if stage == 1:
                return dict(n=n1, h=h1, L=L, La=La, Lb=Lb, p=p1, right=r1, left=l1, R=R1, m=c.m_rs1)
            return dict(n=n2, h=h2, L=L2, La=La2, Lb=Lb2, p=p2, right=r2, left=l2, R=R2, m=c.m_rs2)
        def local(stage, b, row, k):
            if stage == 1:
                return G[b, pl.ds(m16(base + row), k), :].astype(F32) + D[dsl(b), pl.ds(m16(dbase + row), k), :].astype(F32)
            return O1[sl(b), pl.ds(m16(row), k), :] + R1[sl(b), pl.ds(m16(2 * (h1 - 1) * L + row), k), :].astype(F32)
        def staged(stage, b, row, k):
            if stage == 1:
                return D.at[dsl(b), pl.ds(m16(dbase + row), k)]
            return O1b.at[sl(b), pl.ds(m16(row), k)]
        def rs_copy(stage, b, k, direction):
            g = ring(stage)
            n, h, LL, A, Bb = g["n"], g["h"], g["L"], g["La"], g["Lb"]
            s = sl(b)
            if k < h:
                slot = mod(g["p"] + h - k + 1, n) if direction == 0 else mod(g["p"] - h + k, n)
                src = staged(stage, b, slot * LL, LL)
                dst = g["R"].at[s, pl.ds((k - 1) * 2 * LL + direction * LL, LL)]
            elif direction == 0:
                src = staged(stage, b, mod(g["p"] + 1, n) * LL + A, Bb)
                dst = g["R"].at[s, pl.ds((h - 1) * 2 * LL, Bb)]
            else:
                src = staged(stage, b, g["p"] * LL, A)
                dst = g["R"].at[s, pl.ds((h - 1) * 2 * LL + Bb, A)]
            m = g["m"] + 2 * (k - 1) + direction
            return self.copy(src, dst, SS.at[s, m], RS.at[s, m], g["right"] if direction == 0 else g["left"])
        def rs_step(stage, k):
            def f(b):
                g = ring(stage)
                n, h, LL, A, Bb = g["n"], g["h"], g["L"], g["La"], g["Lb"]
                s = sl(b)
                for direction in (0, 1):
                    if k > 1:
                        rs_copy(stage, b, k - 1, direction).wait()
                    slot = mod(g["p"] + h - k + 1, n) if direction == 0 else mod(g["p"] - h + k, n)
                    rin = (k - 2) * 2 * LL + direction * LL
                    def total(row, at, kk):
                        v = local(stage, b, row, kk)
                        if k > 1:
                            v = v + g["R"][s, pl.ds(m16(rin + at), kk), :].astype(F32)
                        return v
                    def send_part(lo, cnt):
                        def body(i, kk):
                            v = total(slot * LL + lo + i, lo + i, kk)
                            if stage == 1:
                                D[dsl(b), pl.ds(m16(dbase + slot * LL + lo + i), kk), :] = v.astype(BF16)
                            else:
                                O1b[s, pl.ds(m16(slot * LL + lo + i), kk), :] = v.astype(BF16)
                        over_rows(cnt, body)
                    def keep_part(lo, cnt, to):
                        ref = O1 if stage == 1 else O2
                        def body(i, kk):
                            ref[s, pl.ds(m16(to + i), kk), :] = total(slot * LL + lo + i, lo + i, kk)
                        over_rows(cnt, body)
                    if k < h:
                        send_part(0, LL)
                        rs_copy(stage, b, k, direction).start()
                    elif direction == 0:
                        send_part(A, Bb)
                        rs_copy(stage, b, k, direction).start()
                        keep_part(0, A, Bb)
                    else:
                        send_part(0, A)
                        rs_copy(stage, b, k, direction).start()
                        keep_part(A, Bb, 0)
            return f
        def rs_end(stage):
            def f(b):
                for direction in (0, 1):
                    rs_copy(stage, b, ring(stage)["h"], direction).wait()
            return f
        def y_copy(b, k):
            s = sl(b)
            m = c.m_y + k - 1
            return self.copy(Y.at[s, p3], Y.at[s, p3], SS.at[s, m], RS.at[s, m], self.shifted(c.dims[2], k))
        def y_wait(b, k):
            s = sl(b)
            m = c.m_y + k - 1
            return self.copy(Y.at[s, p3], Y.at[s, mod(p3 - k, n3)], SS.at[s, m], RS.at[s, m], self.shifted(c.dims[2], k))
        def y_send(b):
            s = sl(b)
            def body(i, kk):
                v = O2[s, pl.ds(i, kk), :] + R2[s, pl.ds(m16(2 * (h2 - 1) * L2 + i), kk), :].astype(F32)
                Y[s, p3, pl.ds(i, kk), :] = v.astype(BF16)
            over_rows(L2, body)
            for k in range(1, n3):
                y_copy(b, k).start()
        def grow(v):
            return base + mod(p1 * L + La + v, c.S)
        def y_sum(b):
            s = sl(b)
            for k in range(1, n3):
                y_wait(b, k).wait()
            def part(src, cnt, row):
                def body(i, kk):
                    v = Y[s, 0, pl.ds(m16(src + i), kk), :].astype(F32)
                    for j in range(1, n3):
                        v = v + Y[s, j, pl.ds(m16(src + i), kk), :].astype(F32)
                    G[b, pl.ds(m16(row + i), kk), :] = v.astype(BF16)
                over_rows(cnt, body)
            part(0, Lb2, grow(p2 * L2 + La2))
            part(Lb2, La2, grow(mod(p2 + 1, n2) * L2))
        def ag_copy(stage, b, k, direction):
            s = sl(b)
            if stage == 2:
                n, LL, A, Bb, p, right, left, m = n2, L2, La2, Lb2, p2, r2, l2, c.m_ag2
                at = lambda slot, part: grow(slot * L2) + part
            else:
                n, LL, A, Bb, p, right, left, m = n1, L, La, Lb, p1, r1, l1, c.m_ag1
                at = lambda slot, part: base + slot * L + part
            if k == 1:
                row, cnt = (at(mod(p + 1, n), 0), A) if direction == 0 else (at(p, A), Bb)
            else:
                row, cnt = (at(mod(p - (k - 2), n), 0) if direction == 0 else at(mod(p + 1 + (k - 2), n), 0)), LL
            ref = G.at[b, pl.ds(m16(row), cnt)]
            mm = m + 2 * (k - 1) + direction
            return self.copy(ref, ref, SS.at[s, mm], RS.at[s, mm], right if direction == 0 else left)
        def ag_in(stage, b, k, direction):
            s = sl(b)
            if stage == 2:
                n, LL, A, Bb, p, right, left, m = n2, L2, La2, Lb2, p2, r2, l2, c.m_ag2
                at = lambda slot, part: grow(slot * L2) + part
            else:
                n, LL, A, Bb, p, right, left, m = n1, L, La, Lb, p1, r1, l1, c.m_ag1
                at = lambda slot, part: base + slot * L + part
            if k == 1:
                row, cnt = (at(p, 0), A) if direction == 0 else (at(mod(p + 1, n), A), Bb)
            else:
                row, cnt = (at(mod(p - 1 - (k - 2), n), 0) if direction == 0 else at(mod(p + 2 + (k - 2), n), 0)), LL
            ref = G.at[b, pl.ds(m16(row), cnt)]
            mm = m + 2 * (k - 1) + direction
            return self.copy(ref, ref, SS.at[s, mm], RS.at[s, mm], right if direction == 0 else left)
        def ag_wait(stage, b, k):
            for direction in (0, 1):
                ag_copy(stage, b, k, direction).wait_send()
                ag_in(stage, b, k, direction).wait_recv()
        def ag_start(stage, b, k):
            for direction in (0, 1):
                ag_copy(stage, b, k, direction).start()
        def pair(b):
            s = sl(b)
            ref = G.at[b, pl.ds(m16(base), c.S)]
            return self.copy(ref, ref, SS.at[s, c.m_pair], RS.at[s, c.m_pair], self.partner)
        def pair_in(b):
            s = sl(b)
            ref = G.at[b, pl.ds(m16(self.other + c.off), c.S)]
            return self.copy(ref, ref, SS.at[s, c.m_pair], RS.at[s, c.m_pair], self.partner)

        out = []
        for k in range(1, h1 + 1):
            out.append(rs_step(1, k))
        for k in range(1, h2 + 1):
            if k == 1:
                out.append(lambda b: (rs_end(1)(b), rs_step(2, 1)(b)))
            else:
                out.append(rs_step(2, k))
        out.append(lambda b: (rs_end(2)(b), y_send(b)))
        out.append(lambda b: (y_sum(b), ag_start(2, b, 1)))
        for k in range(2, h2 + 1):
            out.append(lambda b, k=k: (ag_wait(2, b, k - 1), ag_start(2, b, k)))
        out.append(lambda b: (ag_wait(2, b, h2), ag_start(1, b, 1)))
        for k in range(2, h1 + 1):
            out.append(lambda b, k=k: (ag_wait(1, b, k - 1), ag_start(1, b, k)))
        out.append(lambda b: (ag_wait(1, b, h1), pair(b).start()))
        out.append(lambda b: (pair(b).wait_send(), pair_in(b).wait_recv()))
        return out


TOK, DIM, FF = 1024, 768, 3072
TF = 256
NT = FF // TF
PARTS = 3
K = NT // PARTS
HALF = 512

def dot(a, b):
    return jnp.dot(a, b, preferred_element_type=F32)
def dot_nt(a, b):
    return lax.dot_general(a, b, (((1,), (1,)), ((), ())), preferred_element_type=F32)

OFFS = {
    "A": [0, 1, 3, 4, 5, 6, 7, 8, 9, 10, 11, 12, 13, 14, 16, 17],
    "B": [0, 1, 3, 4, 5, 6, 7, 8, 9, 10, 11, 12, 13, 14, 16, 17],
    "C": [0, 1, 2, 3, 4, 6, 7, 8, 9, 10, 11, 12, 13, 14, 16, 17],
}

def mega(comm, x_hbm, dy_hbm, wg_hbm, wu_hbm, wd_hbm, o_hbm, A, AT, DY, DYT, H, ACC, TH, TG, TU, WG, WU, WD, wsem, xsem, osem, *cs):
    B = comm.B
    comm.setup(cs)
    G = comm.G
    def wcopies(u):
        q = lax.div(u, NT)
        layer = lax.rem(q, 2)
        j = lax.rem(u, NT)
        s = lax.rem(u, 2)
        f = pl.multiple_of(j * TF, TF)
        return (pltpu.make_async_copy(wg_hbm.at[layer, :, pl.ds(f, TF)], WG.at[s], wsem.at[s, 0]),
                pltpu.make_async_copy(wu_hbm.at[layer, :, pl.ds(f, TF)], WU.at[s], wsem.at[s, 1]),
                pltpu.make_async_copy(wd_hbm.at[layer, pl.ds(f, TF), :], WD.at[s], wsem.at[s, 2]))
    def wstart(u):
        for c in wcopies(u):
            c.start()
    def wwait(u):
        for c in wcopies(u):
            c.wait()
    xin = pltpu.make_async_copy(x_hbm, H, xsem.at[0])
    xagain = pltpu.make_async_copy(x_hbm, A, xsem.at[0])
    dyin = pltpu.make_async_copy(dy_hbm, DY, xsem.at[1])
    xin.start(); dyin.start(); wstart(0)
    comm.barrier()

    def rows_of(i, n):
        return pl.ds(pl.multiple_of(i * n, n), n)
    def each(n, body):
        def step(i, _):
            body(rows_of(i, n))
            return 0
        lax.fori_loop(0, TOK // n, step, 0)
    def norm(src, r):
        wide = src[r, :].astype(F32)
        scale = lax.rsqrt(jnp.mean(wide * wide, -1, keepdims=True) + 1e-6)
        return (wide * scale).astype(BF16)
    def zero(r):
        ACC[r, :] = jnp.zeros((r.size, DIM), F32)

    xin.wait()
    def first(r):
        A[r, :] = norm(H, r)
        zero(r)
    each(128, first)

    def forward(u, _):
        s = lax.rem(u, 2)
        wwait(u)
        wstart(u + 1)
        def half(r):
            a = A[r, :]
            gate = dot(a, WG[s])
            up = dot(a, WU[s])
            hid = (gate * jax.nn.sigmoid(gate) * up).astype(BF16)
            ACC[r, :] += dot(hid, WD[s])
        for i in range(TOK // HALF):
            half(pl.ds(i * HALF, HALF))
        return 0
    lax.fori_loop(0, NT, forward, 0)
    dyin.wait()
    def between(r):
        H[r, :] = (H[r, :].astype(F32) + ACC[r, :].astype(BF16).astype(F32)).astype(BF16)
        a = norm(H, r)
        A[r, :] = a
        AT[:, r] = a.T
        DYT[:, r] = DY[r, :].T
        zero(r)
    each(128, between)

    def backward(u, t, want_input):
        s = lax.rem(u, 2)
        b = lax.div(t, K)
        jt = lax.rem(t, K)
        wwait(u)
        @pl.when(u + 1 < 3 * NT)
        def _():
            wstart(u + 1)
        for i in range(TOK // HALF):
            r = pl.ds(i * HALF, HALF)
            a = A[r, :]
            gate = dot(a, WG[s])
            up = dot(a, WU[s])
            dh = dot_nt(DY[r, :], WD[s]).astype(BF16).astype(F32)
            sig = jax.nn.sigmoid(gate)
            act = gate * sig
            TH[r, :] = (act * up).astype(BF16)
            du = (dh * act).astype(BF16)
            dg = (dh * up * (sig * (1.0 + gate * (1.0 - sig)))).astype(BF16)
            TU[r, :] = du
            TG[r, :] = dg
            if want_input:
                ACC[r, :] += dot_nt(dg, WG[s]) + dot_nt(du, WU[s])
        for mat, (lhs, rhs) in enumerate(((AT, TG), (AT, TU), (DYT, TH))):
            d = dot(lhs[...], rhs[...]).astype(BF16)
            for k in range(TF // LANES):
                row = (mat * (K * TF // LANES) + jt * (TF // LANES) + k) * DIM
                G[b, pl.ds(m16(row), DIM), :] = d[:, k * LANES:(k + 1) * LANES]

    def middle():
        xagain.start()
        def body(r):
            da = ACC[r, :].astype(BF16).astype(F32)
            wide = H[r, :].astype(F32)
            scale = lax.rsqrt(jnp.mean(wide * wide, -1, keepdims=True) + 1e-6)
            ds = jnp.sum(da * wide, -1, keepdims=True)
            dwide = da * scale - wide * (ds * scale * scale * scale * (1.0 / DIM))
            d = (DY[r, :].astype(F32) + dwide.astype(BF16).astype(F32)).astype(BF16)
            DY[r, :] = d
            DYT[:, r] = d.T
        each(128, body)
        xagain.wait()
        def again(r):
            a = norm(A, r)
            A[r, :] = a
            AT[:, r] = a.T
        each(128, again)

    store = lambda b: pltpu.make_async_copy(G.at[b], o_hbm.at[b], osem.at[b])
    phases = comm.phases()
    events = []
    for ph, fns in enumerate(phases):
        if ph == 0:
            events += [(0, f) for f in fns]
        else:
            cols = [c.name for c in comm.colors]
            fs = list(fns)
            if ph == 1:
                events.append((1, fs.pop(0)))
            for name, f in zip(cols, fs):
                events.append((OFFS[name][ph], f))
    last = max(o for o, _ in events)
    events.append((last, lambda b: store(b).start()))
    depth = last // K + 1
    def tick(t):
        it = lax.div(t, K) - 1
        for sub in range(K):
            if not any(o % K == sub for o, _ in events):
                continue
            @pl.when(lax.rem(t, K) == sub)
            def _():
                for i in reversed(range(depth)):
                    fs = [f for o, f in events if o == sub + K * i]
                    if not fs:
                        continue
                    b = it - i
                    @pl.when((b >= 0) & (b < B))
                    def _():
                        for f in fs:
                            f(b)
    def step(t, _):
        tick(t)
        @pl.when(t < NT)
        def _():
            backward(t + NT, t, True)
        @pl.when(t == NT)
        def _():
            middle()
        @pl.when((t >= NT) & (t < 2 * NT))
        def _():
            backward(t + NT, t, False)
        return 0
    lax.fori_loop(0, K * B + last + 1, step, 0)
    def fin(b, _):
        store(b).wait()
        return 0
    lax.fori_loop(0, B, fin, 0)

def gradients(comm, x, dy, wg, wu, wd, vmem=66_900_000):
    V = pltpu.VMEM
    scratch = [V((TOK, DIM), BF16), V((DIM, TOK), BF16), V((TOK, DIM), BF16), V((DIM, TOK), BF16), V((TOK, DIM), BF16), V((TOK, DIM), F32),
               V((TOK, TF), BF16), V((TOK, TF), BF16), V((TOK, TF), BF16),
               V((2, DIM, TF), BF16), V((2, DIM, TF), BF16), V((2, TF, DIM), BF16),
               pltpu.SemaphoreType.DMA((2, 3)), pltpu.SemaphoreType.DMA((2,)), pltpu.SemaphoreType.DMA((comm.B,))]
    return pl.pallas_call(
        functools.partial(mega, comm),
        out_shape=jax.ShapeDtypeStruct((comm.B, comm.TB, LANES), BF16),
        in_specs=[pl.BlockSpec(memory_space=pl.ANY)] * 5, out_specs=pl.BlockSpec(memory_space=pl.ANY),
        scratch_shapes=scratch + comm.scratch(),
        compiler_params=pltpu.CompilerParams(collective_id=0, has_side_effects=True, vmem_limit_bytes=vmem),
    )(x, dy, wg, wu, wd)

def adam_kernel(turned, w, m, v, *refs):
    gs, (w2, m2, v2) = refs[:-3], refs[-3:]
    for k, g in enumerate(gs):
        gv = g[0].astype(F32)
        if turned:
            gv = gv.T
            at = (0, pl.ds(k * LANES, LANES), slice(None))
        else:
            at = (0, slice(None), pl.ds(k * LANES, LANES))
        mm = 0.9 * m[at] + 0.1 * gv
        vv = 0.95 * v[at] + 0.05 * gv * gv
        ww = w[at].astype(F32)
        step = mm * lax.rsqrt(vv + 1e-8) + 0.1 * ww
        w2[at] = (ww - 0.02 * step).astype(BF16)
        m2[at] = mm
        v2[at] = vv

def adam(which, w, m, v, g, c=2):
    turned = which == 2
    wide = c * LANES
    per = FF // PARTS // wide
    if turned:
        spec = pl.BlockSpec((1, wide, DIM), lambda l, i: (l, i, 0))
    else:
        spec = pl.BlockSpec((1, DIM, wide), lambda l, i: (l, 0, i))
    def gspec(k):
        def index(l, i):
            return ((1 - l) * PARTS + i // per, which * (FF // PARTS // LANES) + (i % per) * c + k, 0)
        return pl.BlockSpec((1, DIM, LANES), index)
    return pl.pallas_call(
        functools.partial(adam_kernel, turned),
        grid=(2, FF // wide),
        out_shape=(jax.ShapeDtypeStruct(w.shape, BF16), jax.ShapeDtypeStruct(m.shape, F32), jax.ShapeDtypeStruct(v.shape, F32)),
        in_specs=[spec] * 3 + [gspec(k) for k in range(c)], out_specs=(spec,) * 3,
        compiler_params=pltpu.CompilerParams(vmem_limit_bytes=60_000_000),
    )(w, m, v, *([g] * c))
TILE = 16
COLORS = (("A", 224 * TILE, "xzy"), ("B", 224 * TILE, "yzx"), ("C", 128 * TILE, "zxy"))
SIZES = {"x": 4, "y": 4, "z": 8}
def make_comm():
    return Comm(SIZES, COLORS, 2 * PARTS, 2, 3)

def train_step(comm, x, dy, *arrays):
    weights, m, v = (arrays[i:i + 3] for i in (0, 3, 6))
    g = gradients(comm, x[0], dy[0], *weights)
    new = [adam(i, weights[i], m[i], v[i], g) for i in range(3)]
    return tuple(one[which] for which in range(3) for one in new)


def solution(mesh):
    comm = make_comm()
    return jax.shard_map(
        functools.partial(train_step, comm),
        mesh=mesh,
        in_specs=(P(("rep", "dp"), None, None),) * 2 + (P(None, None, None),) * 9,
        out_specs=(P("rep", None, None),) * 9,
        check_vma=False,
    )
```

```python
import functools
import jax
import jax.numpy as jnp
from jax import lax
from jax.experimental import pallas as pl
from jax.experimental.pallas import tpu as pltpu
from jax.sharding import PartitionSpec as P
MESH = pl.DeviceIdType.MESH
F32, BF16 = jnp.float32, jnp.bfloat16
LANES = 128

def chunk_of(n, cap=256):
    best = 16
    for c in range(16, cap + 1, 16):
        if n % c == 0:
            best = c
    return best

def over_rows(n, body, cap=256):
    c = chunk_of(n, cap)
    if n == c:
        body(0, c)
    else:
        def step(i, _):
            body(pl.multiple_of(i * c, 16), c)
            return 0
        lax.fori_loop(0, n // c, step, 0)

class Color:
    def __init__(self, name, off, S, dims, n):
        self.name, self.off, self.S, self.dims = name, off, S, dims
        self.n1, self.n2, self.n3 = (n[d] for d in dims)
        self.L = S // self.n1
        self.La = (self.L // 2) // 16 * 16
        self.Lb = self.L - self.La
        self.L2 = self.L // self.n2
        self.La2 = (self.L2 // 2) // 16 * 16
        self.Lb2 = self.L2 - self.La2
        assert S % (self.n1 * self.n2 * 16) == 0 and self.Lb % self.L2 == 0 and self.La2 > 0, (S, self.L, self.L2)
        h1, h2 = self.n1 // 2, self.n2 // 2
        self.h1, self.h2 = h1, h2
        self.m_rs1, self.m_rs2 = 0, 2 * h1
        self.m_y = self.m_rs2 + 2 * h2
        self.m_ag2 = self.m_y + self.n3 - 1
        self.m_ag1 = self.m_ag2 + 2 * h2
        self.m_pair = self.m_ag1 + 2 * h1
        self.nmsg = self.m_pair + 1
    def scratch(self, N):
        return [pltpu.VMEM((N["R1"], (self.n1 - 1) * self.L, LANES), BF16),
                pltpu.VMEM((N["O1"], self.L, LANES), F32),
                pltpu.VMEM((N["O1b"], self.L, LANES), BF16),
                pltpu.VMEM((N["R2"], (self.n2 - 1) * self.L2, LANES), BF16),
                pltpu.VMEM((N["O2"], self.L2, LANES), F32),
                pltpu.VMEM((N["Y"], self.n3, self.L2, LANES), BF16),
                pltpu.SemaphoreType.DMA((N["S"], self.nmsg)), pltpu.SemaphoreType.DMA((N["S"], self.nmsg))]

def m16(v):
    return pl.multiple_of(v, 16)

class Comm:
    def __init__(self, n, cfg, B, slots):
        self.n, self.B, self.N = n, B, slots
        self.ND = slots["D"]
        off, self.colors = 0, []
        for name, rows, dims in cfg:
            self.colors.append(Color(name, off, rows, dims, n)); off += rows
        self.HB, self.TB = off, 2 * off
    def scratch(self):
        out = [pltpu.VMEM((self.ND, self.HB, LANES), BF16),
               pltpu.SemaphoreType.DMA((self.ND,)), pltpu.SemaphoreType.DMA((self.ND,))]
        for c in self.colors:
            out += c.scratch(self.N)
        return out
    def setup(self, G, scratch):
        self.G = G
        n = self.n
        me = lax.axis_index("dp")
        core = lax.rem(me, 2); z = lax.rem(lax.div(me, 2), n["z"])
        y = lax.rem(lax.div(me, 2 * n["z"]), n["y"]); x = lax.div(me, 2 * n["z"] * n["y"])
        self.pos = {"x": x, "y": y, "z": z}
        self.core = core
        stride = {"x": 2 * n["z"] * n["y"], "y": 2 * n["z"], "z": 2}
        def shifted(d, k):
            q = lax.rem(self.pos[d] + k + n[d], n[d])
            return me + (q - self.pos[d]) * stride[d]
        self.shifted = shifted
        self.partner = me + 1 - 2 * core
        self.D, self.ds, self.dr = scratch[:3]
        self.bufs = {}
        rest = scratch[3:]
        for i, c in enumerate(self.colors):
            self.bufs[c.name] = rest[8 * i:8 * i + 8]
        self.mine = core * self.HB
        self.other = (1 - core) * self.HB
    def barrier(self):
        n = self.n
        peers = [self.partner]
        need = {d: set() for d in "xyz"}
        for c in self.colors:
            for d in c.dims[:2]:
                need[d] |= {1 % n[d], (n[d] - 1) % n[d]}
            need[c.dims[2]] |= set(range(1, n[c.dims[2]]))
        for d in "xyz":
            for k in sorted(need[d]):
                if k:
                    peers.append(self.shifted(d, k))
        sem = pltpu.get_barrier_semaphore()
        for p in peers:
            pl.semaphore_signal(sem, inc=1, device_id={"dp": p}, device_id_type=MESH)
        pl.semaphore_wait(sem, len(peers))
    def copy(self, src, dst, ss, rs, dev):
        return pltpu.make_async_remote_copy(src_ref=src, dst_ref=dst, send_sem=ss, recv_sem=rs, device_id={"dp": dev}, device_id_type=MESH)

    def pair_copy(self, b):
        s = lax.rem(b, self.ND)
        return self.copy(self.G.at[b, pl.ds(m16(self.other), self.HB)], self.D.at[s], self.ds.at[s], self.dr.at[s], self.partner)
    def phases(self):
        out = [[lambda b: self.pair_copy(b).start()], [lambda b: self.pair_copy(b).wait()]]
        per = [self.color_phases(c) for c in self.colors]
        depth = max(len(p) for p in per)
        out += [[] for _ in range(depth - 1)]
        for p in per:
            for i, f in enumerate(p):
                out[1 + i].append(f)
        return out

    def color_phases(self, c):
        G, D = self.G, self.D
        R1, O1, O1b, R2, O2, Y, SS, RS = self.bufs[c.name]
        N = self.N
        p1, p2, p3 = (self.pos[d] for d in c.dims)
        r1, l1 = self.shifted(c.dims[0], 1), self.shifted(c.dims[0], -1)
        r2, l2 = self.shifted(c.dims[1], 1), self.shifted(c.dims[1], -1)
        n1, n2, n3, h1, h2 = c.n1, c.n2, c.n3, c.h1, c.h2
        L, La, Lb, L2, La2, Lb2 = c.L, c.La, c.Lb, c.L2, c.La2, c.Lb2
        mod = lambda v, n: lax.rem(v + 4 * n, n)
        base = self.mine + c.off
        dbase = c.off
        at_ = lambda name: (lambda b: lax.rem(b, N[name]))
        sR1, sO1, sO1b, sR2, sO2, sY, sl, dsl = (at_(k) for k in ("R1", "O1", "O1b", "R2", "O2", "Y", "S", "D"))

        def ring(stage):
            if stage == 1:
                return dict(n=n1, h=h1, L=L, La=La, Lb=Lb, p=p1, right=r1, left=l1, R=R1, sR=sR1, m=c.m_rs1)
            return dict(n=n2, h=h2, L=L2, La=La2, Lb=Lb2, p=p2, right=r2, left=l2, R=R2, sR=sR2, m=c.m_rs2)
        def local(stage, b, row, k):
            if stage == 1:
                return G[b, pl.ds(m16(base + row), k), :].astype(F32) + D[dsl(b), pl.ds(m16(dbase + row), k), :].astype(F32)
            return O1[sO1(b), pl.ds(m16(row), k), :] + R1[sR1(b), pl.ds(m16(2 * (h1 - 1) * L + row), k), :].astype(F32)
        def staged(stage, b, row, k):
            if stage == 1:
                return D.at[dsl(b), pl.ds(m16(dbase + row), k)]
            return O1b.at[sO1b(b), pl.ds(m16(row), k)]
        def rs_copy(stage, b, k, direction):
            g = ring(stage)
            n, h, LL, A, Bb = g["n"], g["h"], g["L"], g["La"], g["Lb"]
            s = sl(b)
            if k < h:
                slot = mod(g["p"] + h - k + 1, n) if direction == 0 else mod(g["p"] - h + k, n)
                src = staged(stage, b, slot * LL, LL)
                dst = g["R"].at[g["sR"](b), pl.ds((k - 1) * 2 * LL + direction * LL, LL)]
            elif direction == 0:
                src = staged(stage, b, mod(g["p"] + 1, n) * LL + A, Bb)
                dst = g["R"].at[g["sR"](b), pl.ds((h - 1) * 2 * LL, Bb)]
            else:
                src = staged(stage, b, g["p"] * LL, A)
                dst = g["R"].at[g["sR"](b), pl.ds((h - 1) * 2 * LL + Bb, A)]
            m = g["m"] + 2 * (k - 1) + direction
            return self.copy(src, dst, SS.at[s, m], RS.at[s, m], g["right"] if direction == 0 else g["left"])
        def rs_step(stage, k):
            def f(b):
                g = ring(stage)
                n, h, LL, A, Bb = g["n"], g["h"], g["L"], g["La"], g["Lb"]
                s = sl(b)
                for direction in (0, 1):
                    if k > 1:
                        rs_copy(stage, b, k - 1, direction).wait()
                    slot = mod(g["p"] + h - k + 1, n) if direction == 0 else mod(g["p"] - h + k, n)
                    rin = (k - 2) * 2 * LL + direction * LL
                    def total(row, at, kk):
                        v = local(stage, b, row, kk)
                        if k > 1:
                            v = v + g["R"][g["sR"](b), pl.ds(m16(rin + at), kk), :].astype(F32)
                        return v
                    def send_part(lo, cnt):
                        def body(i, kk):
                            v = total(slot * LL + lo + i, lo + i, kk)
                            if stage == 1:
                                D[dsl(b), pl.ds(m16(dbase + slot * LL + lo + i), kk), :] = v.astype(BF16)
                            else:
                                O1b[sO1b(b), pl.ds(m16(slot * LL + lo + i), kk), :] = v.astype(BF16)
                        over_rows(cnt, body)
                    def keep_part(lo, cnt, to):
                        ref, so = (O1, sO1(b)) if stage == 1 else (O2, sO2(b))
                        def body(i, kk):
                            ref[so, pl.ds(m16(to + i), kk), :] = total(slot * LL + lo + i, lo + i, kk)
                        over_rows(cnt, body)
                    if k < h:
                        send_part(0, LL)
                        rs_copy(stage, b, k, direction).start()
                    elif direction == 0:
                        send_part(A, Bb)
                        rs_copy(stage, b, k, direction).start()
                        keep_part(0, A, Bb)
                    else:
                        send_part(0, A)
                        rs_copy(stage, b, k, direction).start()
                        keep_part(A, Bb, 0)
            return f
        def rs_end(stage):
            def f(b):
                for direction in (0, 1):
                    rs_copy(stage, b, ring(stage)["h"], direction).wait()
            return f
        def y_copy(b, k):
            s = sl(b)
            m = c.m_y + k - 1
            return self.copy(Y.at[sY(b), p3], Y.at[sY(b), p3], SS.at[s, m], RS.at[s, m], self.shifted(c.dims[2], k))
        def y_wait(b, k):
            s = sl(b)
            m = c.m_y + k - 1
            return self.copy(Y.at[sY(b), p3], Y.at[sY(b), mod(p3 - k, n3)], SS.at[s, m], RS.at[s, m], self.shifted(c.dims[2], k))
        def y_send(b):
            s = sl(b)
            def body(i, kk):
                v = O2[sO2(b), pl.ds(i, kk), :] + R2[sR2(b), pl.ds(m16(2 * (h2 - 1) * L2 + i), kk), :].astype(F32)
                Y[sY(b), p3, pl.ds(i, kk), :] = v.astype(BF16)
            over_rows(L2, body)
            for k in range(1, n3):
                y_copy(b, k).start()
        def grow(v):
            return base + mod(p1 * L + La + v, c.S)
        def y_sum(b):
            s = sl(b)
            for k in range(1, n3):
                y_wait(b, k).wait()
            def part(src, cnt, row):
                def body(i, kk):
                    v = Y[sY(b), 0, pl.ds(m16(src + i), kk), :].astype(F32)
                    for j in range(1, n3):
                        v = v + Y[sY(b), j, pl.ds(m16(src + i), kk), :].astype(F32)
                    G[b, pl.ds(m16(row + i), kk), :] = v.astype(BF16)
                over_rows(cnt, body)
            part(0, Lb2, grow(p2 * L2 + La2))
            part(Lb2, La2, grow(mod(p2 + 1, n2) * L2))
        def ag_copy(stage, b, k, direction):
            s = sl(b)
            if stage == 2:
                n, LL, A, Bb, p, right, left, m = n2, L2, La2, Lb2, p2, r2, l2, c.m_ag2
                at = lambda slot, part: grow(slot * L2) + part
            else:
                n, LL, A, Bb, p, right, left, m = n1, L, La, Lb, p1, r1, l1, c.m_ag1
                at = lambda slot, part: base + slot * L + part
            if k == 1:
                row, cnt = (at(mod(p + 1, n), 0), A) if direction == 0 else (at(p, A), Bb)
            else:
                row, cnt = (at(mod(p - (k - 2), n), 0) if direction == 0 else at(mod(p + 1 + (k - 2), n), 0)), LL
            ref = G.at[b, pl.ds(m16(row), cnt)]
            mm = m + 2 * (k - 1) + direction
            return self.copy(ref, ref, SS.at[s, mm], RS.at[s, mm], right if direction == 0 else left)
        def ag_in(stage, b, k, direction):
            s = sl(b)
            if stage == 2:
                n, LL, A, Bb, p, right, left, m = n2, L2, La2, Lb2, p2, r2, l2, c.m_ag2
                at = lambda slot, part: grow(slot * L2) + part
            else:
                n, LL, A, Bb, p, right, left, m = n1, L, La, Lb, p1, r1, l1, c.m_ag1
                at = lambda slot, part: base + slot * L + part
            if k == 1:
                row, cnt = (at(p, 0), A) if direction == 0 else (at(mod(p + 1, n), A), Bb)
            else:
                row, cnt = (at(mod(p - 1 - (k - 2), n), 0) if direction == 0 else at(mod(p + 2 + (k - 2), n), 0)), LL
            ref = G.at[b, pl.ds(m16(row), cnt)]
            mm = m + 2 * (k - 1) + direction
            return self.copy(ref, ref, SS.at[s, mm], RS.at[s, mm], right if direction == 0 else left)
        def ag_wait(stage, b, k):
            for direction in (0, 1):
                ag_copy(stage, b, k, direction).wait_send()
                ag_in(stage, b, k, direction).wait_recv()
        def ag_start(stage, b, k):
            for direction in (0, 1):
                ag_copy(stage, b, k, direction).start()
        def pair(b):
            s = sl(b)
            ref = G.at[b, pl.ds(m16(base), c.S)]
            return self.copy(ref, ref, SS.at[s, c.m_pair], RS.at[s, c.m_pair], self.partner)
        def pair_in(b):
            s = sl(b)
            ref = G.at[b, pl.ds(m16(self.other + c.off), c.S)]
            return self.copy(ref, ref, SS.at[s, c.m_pair], RS.at[s, c.m_pair], self.partner)

        out = []
        for k in range(1, h1 + 1):
            out.append(rs_step(1, k))
        for k in range(1, h2 + 1):
            if k == 1:
                out.append(lambda b: (rs_end(1)(b), rs_step(2, 1)(b)))
            else:
                out.append(rs_step(2, k))
        out.append(lambda b: (rs_end(2)(b), y_send(b)))
        out.append(lambda b: (y_sum(b), ag_start(2, b, 1)))
        for k in range(2, h2 + 1):
            out.append(lambda b, k=k: (ag_wait(2, b, k - 1), ag_start(2, b, k)))
        out.append(lambda b: (ag_wait(2, b, h2), ag_start(1, b, 1)))
        for k in range(2, h1 + 1):
            out.append(lambda b, k=k: (ag_wait(1, b, k - 1), ag_start(1, b, k)))
        out.append(lambda b: (ag_wait(1, b, h1), pair(b).start()))
        out.append(lambda b: (pair(b).wait_send(), pair_in(b).wait_recv()))
        return out


TOK, DIM, FF = 1024, 768, 3072
TF = 256
NT = FF // TF
PARTS = 6
K = NT // PARTS
HALF = 512

def dot(a, b):
    return jnp.dot(a, b, preferred_element_type=F32)
def dot_nt(a, b):
    return lax.dot_general(a, b, (((1,), (1,)), ((), ())), preferred_element_type=F32)

OFFS = {
    "A": [0, 1, 4, 5, 6, 7, 8, 9, 10, 11, 12, 13, 14, 15, 18, 19],
    "B": [0, 1, 3, 4, 5, 6, 7, 8, 9, 10, 11, 12, 13, 14, 16, 17],
    "C": [0, 1, 2, 3, 5, 7, 8, 9, 10, 11, 12, 13, 14, 15, 17, 18],
}
SLOTS = {"R1": 4, "O1": 2, "O1b": 2, "R2": 3, "O2": 2, "Y": 2, "D": 5, "S": 12}

def mega(comm, x_hbm, dy_hbm, wg_hbm, wu_hbm, wd_hbm, G, A, AT, DY, DYT, H, ACC, TH, TG, TU, WG, WU, WD, wsem, xsem, *cs):
    B = comm.B
    comm.setup(G, cs)
    def wcopies(u):
        q = lax.div(u, NT)
        layer = lax.rem(q, 2)
        j = lax.rem(u, NT)
        s = lax.rem(u, 2)
        f = pl.multiple_of(j * TF, TF)
        return (pltpu.make_async_copy(wg_hbm.at[layer, :, pl.ds(f, TF)], WG.at[s], wsem.at[s, 0]),
                pltpu.make_async_copy(wu_hbm.at[layer, :, pl.ds(f, TF)], WU.at[s], wsem.at[s, 1]),
                pltpu.make_async_copy(wd_hbm.at[layer, pl.ds(f, TF), :], WD.at[s], wsem.at[s, 2]))
    def wstart(u):
        for c in wcopies(u):
            c.start()
    def wwait(u):
        for c in wcopies(u):
            c.wait()
    xin = pltpu.make_async_copy(x_hbm, H, xsem.at[0])
    xagain = pltpu.make_async_copy(x_hbm, A, xsem.at[0])
    dyin = pltpu.make_async_copy(dy_hbm, DY, xsem.at[1])
    xin.start(); dyin.start(); wstart(0)
    comm.barrier()

    def rows_of(i, n):
        return pl.ds(pl.multiple_of(i * n, n), n)
    def each(n, body):
        def step(i, _):
            body(rows_of(i, n))
            return 0
        lax.fori_loop(0, TOK // n, step, 0)
    def norm(src, r):
        wide = src[r, :].astype(F32)
        scale = lax.rsqrt(jnp.mean(wide * wide, -1, keepdims=True) + 1e-6)
        return (wide * scale).astype(BF16)
    def zero(r):
        ACC[r, :] = jnp.zeros((r.size, DIM), F32)

    xin.wait()
    def first(r):
        A[r, :] = norm(H, r)
        zero(r)
    each(128, first)

    def forward(u, _):
        s = lax.rem(u, 2)
        wwait(u)
        wstart(u + 1)
        def half(r):
            a = A[r, :]
            gate = dot(a, WG[s])
            up = dot(a, WU[s])
            hid = (gate * jax.nn.sigmoid(gate) * up).astype(BF16)
            ACC[r, :] += dot(hid, WD[s])
        for i in range(TOK // HALF):
            half(pl.ds(i * HALF, HALF))
        return 0
    lax.fori_loop(0, NT, forward, 0)
    dyin.wait()
    def between(r):
        H[r, :] = (H[r, :].astype(F32) + ACC[r, :].astype(BF16).astype(F32)).astype(BF16)
        a = norm(H, r)
        A[r, :] = a
        AT[:, r] = a.T
        DYT[:, r] = DY[r, :].T
        zero(r)
    each(128, between)

    def backward(u, t, want_input):
        s = lax.rem(u, 2)
        b = lax.div(t, K)
        jt = lax.rem(t, K)
        wwait(u)
        @pl.when(u + 1 < 3 * NT)
        def _():
            wstart(u + 1)
        for i in range(TOK // HALF):
            r = pl.ds(i * HALF, HALF)
            a = A[r, :]
            gate = dot(a, WG[s])
            up = dot(a, WU[s])
            dh = dot_nt(DY[r, :], WD[s]).astype(BF16).astype(F32)
            sig = jax.nn.sigmoid(gate)
            act = gate * sig
            TH[r, :] = (act * up).astype(BF16)
            du = (dh * act).astype(BF16)
            dg = (dh * up * (sig * (1.0 + gate * (1.0 - sig)))).astype(BF16)
            TU[r, :] = du
            TG[r, :] = dg
            if want_input:
                ACC[r, :] += dot_nt(dg, WG[s]) + dot_nt(du, WU[s])
        for mat, (lhs, rhs) in enumerate(((AT, TG), (AT, TU), (DYT, TH))):
            d = dot(lhs[...], rhs[...]).astype(BF16)
            for k in range(TF // LANES):
                row = (mat * (K * TF // LANES) + jt * (TF // LANES) + k) * DIM
                G[b, pl.ds(m16(row), DIM), :] = d[:, k * LANES:(k + 1) * LANES]

    def middle():
        xagain.start()
        def body(r):
            da = ACC[r, :].astype(BF16).astype(F32)
            wide = H[r, :].astype(F32)
            scale = lax.rsqrt(jnp.mean(wide * wide, -1, keepdims=True) + 1e-6)
            ds = jnp.sum(da * wide, -1, keepdims=True)
            dwide = da * scale - wide * (ds * scale * scale * scale * (1.0 / DIM))
            d = (DY[r, :].astype(F32) + dwide.astype(BF16).astype(F32)).astype(BF16)
            DY[r, :] = d
            DYT[:, r] = d.T
        each(128, body)
        xagain.wait()
        def again(r):
            a = norm(A, r)
            A[r, :] = a
            AT[:, r] = a.T
        each(128, again)

    phases = comm.phases()
    events = []
    for ph, fns in enumerate(phases):
        if ph == 0:
            events += [(0, f) for f in fns]
        else:
            cols = [c.name for c in comm.colors]
            fs = list(fns)
            if ph == 1:
                events.append((1, fs.pop(0)))
            for name, f in zip(cols, fs):
                events.append((OFFS[name][ph], f))
    last = max(o for o, _ in events)
    depth = last // K + 1
    def tick(t):
        it = lax.div(t, K) - 1
        for sub in range(K):
            if not any(o % K == sub for o, _ in events):
                continue
            @pl.when(lax.rem(t, K) == sub)
            def _():
                for i in reversed(range(depth)):
                    fs = [f for o, f in events if o == sub + K * i]
                    if not fs:
                        continue
                    b = it - i
                    @pl.when((b >= 0) & (b < B))
                    def _():
                        for f in fs:
                            f(b)
    def step(t, _):
        tick(t)
        @pl.when(t < NT)
        def _():
            backward(t + NT, t, True)
        @pl.when(t == NT)
        def _():
            middle()
        @pl.when((t >= NT) & (t < 2 * NT))
        def _():
            backward(t + NT, t, False)
        return 0
    lax.fori_loop(0, K * B + last + 1, step, 0)

def gradients(comm, x, dy, wg, wu, wd, vmem=37_000_000):
    V = pltpu.VMEM
    scratch = [V((TOK, DIM), BF16), V((DIM, TOK), BF16), V((TOK, DIM), BF16), V((DIM, TOK), BF16), V((TOK, DIM), BF16), V((TOK, DIM), F32),
               V((TOK, TF), BF16), V((TOK, TF), BF16), V((TOK, TF), BF16),
               V((2, DIM, TF), BF16), V((2, DIM, TF), BF16), V((2, TF, DIM), BF16),
               pltpu.SemaphoreType.DMA((2, 3)), pltpu.SemaphoreType.DMA((2,))]
    return pl.pallas_call(
        functools.partial(mega, comm),
        out_shape=pltpu.VMEM((comm.B, comm.TB, LANES), BF16),
        in_specs=[pl.BlockSpec(memory_space=pl.ANY)] * 5, out_specs=pl.BlockSpec(memory_space=pltpu.VMEM),
        scratch_shapes=scratch + comm.scratch(),
        compiler_params=pltpu.CompilerParams(collective_id=0, has_side_effects=True, vmem_limit_bytes=vmem),
    )(x, dy, wg, wu, wd)

def adam_all(weights, m, v, g, parts, layers=2, wide=256, nbuf=4, g_vmem=True, ahead=2, light=False):
    dim, ff = weights[0].shape[1:]
    c = wide // LANES
    per = ff // parts // wide
    steps = ff // wide
    cols = ff // parts // LANES
    S = layers * steps
    def body(wg, wu, wd, mg, mu, md, vg, vu, vd, gr, owg, owu, owd, omg, omu, omd, ovg, ovu, ovd,
             wb, mb, vb, xw, xm, xv, dwb, dmb, dvb, dxw, dxm, dxv, *rest):
        if g_vmem:
            isem, osem, disem, dosem = rest
        else:
            gb, dgb, isem, osem, disem, dosem = rest
        def where(i):
            l = lax.div(i, steps)
            j = lax.rem(i, steps)
            return l, j, (layers - 1 - l) * parts + lax.div(j, per), lax.rem(j, per) * c
        def side(l, j):
            return (l, slice(None), pl.ds(pl.multiple_of(j * wide, wide), wide))
        def tall(l, j):
            return (l, pl.ds(pl.multiple_of(j * wide, wide), wide), slice(None))
        sets = {
            0: (wg, mg, vg, owg, omg, ovg), 1: (wu, mu, vu, owu, omu, ovu), 2: (wd, md, vd, owd, omd, ovd)}
        def ins(which, i):
            l, j, b, cb = where(i)
            at = tall(l, j) if which == 2 else side(l, j)
            bufs = (dwb, dmb, dvb) if which == 2 else (wb, mb, vb)
            sem = disem if which == 2 else isem
            s = lax.rem(i, nbuf) if which == 2 else lax.rem(i + which * S, nbuf)
            out = [pltpu.make_async_copy(sets[which][k].at[at], bufs[k].at[s], sem.at[s, k]) for k in range(3)]
            if not g_vmem:
                out.append(pltpu.make_async_copy(gr.at[b, pl.ds(pl.multiple_of((which * cols + cb) * dim, dim), c * dim)], (dgb if which == 2 else gb).at[s], sem.at[s, 3]))
            return out
        def outs(which, i):
            l, j, b, cb = where(i)
            at = tall(l, j) if which == 2 else side(l, j)
            bufs = (dxw, dxm, dxv) if which == 2 else (xw, xm, xv)
            sem = dosem if which == 2 else osem
            s = lax.rem(i, 2) if which == 2 else lax.rem(i + which * S, 2)
            return [pltpu.make_async_copy(bufs[k].at[s], sets[which][3 + k].at[at], sem.at[s, k]) for k in range(3)]
        def start(cs):
            for x in cs:
                x.start()
        def wait(cs):
            for x in cs:
                x.wait()
        def compute(which, i):
            l, j, b, cb = where(i)
            down = which == 2
            s = lax.rem(i, nbuf) if down else lax.rem(i + which * S, nbuf)
            so = lax.rem(i, 2) if down else lax.rem(i + which * S, 2)
            w_, m_, v_, ow, om, ov = (dwb, dmb, dvb, dxw, dxm, dxv) if down else (wb, mb, vb, xw, xm, xv)
            for k in range(c):
                for r in range(0, 256 if light else dim, 256):
                    if g_vmem:
                        row = pl.multiple_of((which * cols + cb + k) * dim + r, 128)
                        gv = gr[b, pl.ds(row, 256), :].astype(F32)
                    else:
                        gv = (dgb if down else gb)[s, pl.ds(k * dim + r, 256), :].astype(F32)
                    if down:
                        gv = gv.T
                        at = (pl.ds(k * LANES, LANES), pl.ds(r, 256))
                    else:
                        at = (pl.ds(r, 256), pl.ds(k * LANES, LANES))
                    mm = 0.9 * m_[(s, *at)] + 0.1 * gv
                    vv = 0.95 * v_[(s, *at)] + 0.05 * gv * gv
                    ww = w_[(s, *at)].astype(F32)
                    step = mm * lax.rsqrt(vv + 1e-8) + 0.1 * ww
                    ow[(so, *at)] = (ww - 0.02 * step).astype(BF16)
                    om[(so, *at)] = mm
                    ov[(so, *at)] = vv
        def whole(i, f):
            @pl.when(i < S)
            def _():
                f(0, i)
            @pl.when((i >= S) & (i < 2 * S))
            def _():
                f(1, i - S)
        for i in range(ahead):
            start(ins(0, i))
        def wide_step(i, _):
            whole(i + ahead, lambda w, t: start(ins(w, t)))
            @pl.when(i + ahead >= 2 * S)
            def _():
                start(ins(2, i + ahead - 2 * S))
            whole(i, lambda w, t: wait(ins(w, t)))
            @pl.when(i >= 2)
            def _():
                whole(i - 2, lambda w, t: wait(outs(w, t)))
            whole(i, lambda w, t: (compute(w, t), start(outs(w, t))))
            return 0
        lax.fori_loop(0, 2 * S, wide_step, 0)
        def tall_step(i, _):
            @pl.when(i + ahead < S)
            def _():
                start(ins(2, i + ahead))
            wait(ins(2, i))
            @pl.when(i >= 2)
            def _():
                wait(outs(2, i - 2))
            compute(2, i)
            start(outs(2, i))
            return 0
        lax.fori_loop(0, S, tall_step, 0)
        for i in (S - 2, S - 1):
            wait(outs(1, i))
            wait(outs(2, i))
    V, D = pltpu.VMEM, pltpu.SemaphoreType.DMA
    scratch = []
    for shape in ((dim, wide), (wide, dim)):
        scratch += [V((nbuf, *shape), BF16), V((nbuf, *shape), F32), V((nbuf, *shape), F32), V((2, *shape), BF16), V((2, *shape), F32), V((2, *shape), F32)]
    if not g_vmem:
        scratch += [V((nbuf, c * dim, LANES), BF16)] * 2
    scratch += [D((nbuf, 4)), D((2, 3)), D((nbuf, 4)), D((2, 3))]
    anys = pl.BlockSpec(memory_space=pl.ANY)
    out = pl.pallas_call(
        body,
        out_shape=[jax.ShapeDtypeStruct(x.shape, x.dtype) for x in (*weights, *m, *v)],
        in_specs=[anys] * 9 + [pl.BlockSpec(memory_space=pltpu.VMEM if g_vmem else pl.ANY)],
        out_specs=[anys] * 9, scratch_shapes=scratch,
        compiler_params=pltpu.CompilerParams(vmem_limit_bytes=30_000_000 if g_vmem else 60_000_000),
    )(*weights, *m, *v, pltpu.with_memory_space_constraint(g, pltpu.VMEM) if g_vmem else g)
    return tuple(out)
TILE = 16
COLORS = (("A", 96 * TILE, "xzy"), ("B", 128 * TILE, "yzx"), ("C", 64 * TILE, "zxy"))
SIZES = {"x": 4, "y": 4, "z": 8}
def make_comm():
    return Comm(SIZES, COLORS, 2 * PARTS, SLOTS)

def train_step(comm, x, dy, *arrays):
    weights, m, v = (arrays[i:i + 3] for i in (0, 3, 6))
    g = gradients(comm, x[0], dy[0], *weights)
    return adam_all(weights, m, v, g, PARTS, nbuf=3)


def solution(mesh):
    comm = make_comm()
    return jax.shard_map(
        functools.partial(train_step, comm),
        mesh=mesh,
        in_specs=(P(("rep", "dp"), None, None),) * 2 + (P(None, None, None),) * 9,
        out_specs=(P("rep", None, None),) * 9,
        check_vma=False,
    )
```

```python
import functools
import jax
import jax.numpy as jnp
from jax import lax
from jax.experimental import pallas as pl
from jax.experimental.pallas import tpu as pltpu
from jax.sharding import PartitionSpec as P
MESH = pl.DeviceIdType.MESH
F32, BF16 = jnp.float32, jnp.bfloat16
LANES = 128

def chunk_of(n, cap=256):
    best = 16
    for c in range(16, cap + 1, 16):
        if n % c == 0:
            best = c
    return best

def over_rows(n, body, cap=256):
    c = chunk_of(n, cap)
    if n == c:
        body(0, c)
    else:
        def step(i, _):
            body(pl.multiple_of(i * c, 16), c)
            return 0
        lax.fori_loop(0, n // c, step, 0)

class Color:
    def __init__(self, name, off, S, dims, n):
        self.name, self.off, self.S, self.dims = name, off, S, dims
        self.n1, self.n2, self.n3 = (n[d] for d in dims)
        self.L = S // self.n1
        self.La = (self.L // 2) // 16 * 16
        self.Lb = self.L - self.La
        self.L2 = self.L // self.n2
        self.La2 = (self.L2 // 2) // 16 * 16
        self.Lb2 = self.L2 - self.La2
        assert S % (self.n1 * self.n2 * 16) == 0 and self.Lb % self.L2 == 0 and self.La2 > 0, (S, self.L, self.L2)
        h1, h2 = self.n1 // 2, self.n2 // 2
        self.h1, self.h2 = h1, h2
        self.m_rs1, self.m_rs2 = 0, 2 * h1
        self.m_y = self.m_rs2 + 2 * h2
        self.m_ag2 = self.m_y + self.n3 - 1
        self.m_ag1 = self.m_ag2 + 2 * h2
        self.m_pair = self.m_ag1 + 2 * h1
        self.nmsg = self.m_pair + 1
    def scratch(self, N):
        return [pltpu.VMEM((N["R1"], (self.n1 - 1) * self.L, LANES), BF16),
                pltpu.VMEM((N["O1"], self.L, LANES), F32),
                pltpu.VMEM((N["O1b"], self.L, LANES), BF16),
                pltpu.VMEM((N["R2"], (self.n2 - 1) * self.L2, LANES), BF16),
                pltpu.VMEM((N["O2"], self.L2, LANES), F32),
                pltpu.VMEM((N["Y"], self.n3, self.L2, LANES), BF16),
                pltpu.SemaphoreType.DMA((N["S"], self.nmsg)), pltpu.SemaphoreType.DMA((N["S"], self.nmsg))]

def m16(v):
    return pl.multiple_of(v, 16)

class Comm:
    def __init__(self, n, cfg, B, slots):
        self.n, self.B, self.N = n, B, slots
        self.ND = slots["D"]
        off, self.colors = 0, []
        for name, rows, dims in cfg:
            self.colors.append(Color(name, off, rows, dims, n)); off += rows
        self.HB, self.TB = off, 2 * off
    def scratch(self):
        out = [pltpu.VMEM((self.ND, self.HB, LANES), BF16),
               pltpu.SemaphoreType.DMA((self.ND,)), pltpu.SemaphoreType.DMA((self.ND,))]
        for c in self.colors:
            out += c.scratch(self.N)
        return out
    def setup(self, G, scratch):
        self.G = G
        n = self.n
        me = lax.axis_index("dp")
        core = lax.rem(me, 2); z = lax.rem(lax.div(me, 2), n["z"])
        y = lax.rem(lax.div(me, 2 * n["z"]), n["y"]); x = lax.div(me, 2 * n["z"] * n["y"])
        self.pos = {"x": x, "y": y, "z": z}
        self.core = core
        stride = {"x": 2 * n["z"] * n["y"], "y": 2 * n["z"], "z": 2}
        def shifted(d, k):
            q = lax.rem(self.pos[d] + k + n[d], n[d])
            return me + (q - self.pos[d]) * stride[d]
        self.shifted = shifted
        self.partner = me + 1 - 2 * core
        self.D, self.ds, self.dr = scratch[:3]
        self.bufs = {}
        rest = scratch[3:]
        for i, c in enumerate(self.colors):
            self.bufs[c.name] = rest[8 * i:8 * i + 8]
        self.mine = core * self.HB
        self.other = (1 - core) * self.HB
    def barrier(self):
        n = self.n
        peers = [self.partner]
        need = {d: set() for d in "xyz"}
        for c in self.colors:
            for d in c.dims[:2]:
                need[d] |= {1 % n[d], (n[d] - 1) % n[d]}
            need[c.dims[2]] |= set(range(1, n[c.dims[2]]))
        for d in "xyz":
            for k in sorted(need[d]):
                if k:
                    peers.append(self.shifted(d, k))
        sem = pltpu.get_barrier_semaphore()
        for p in peers:
            pl.semaphore_signal(sem, inc=1, device_id={"dp": p}, device_id_type=MESH)
        pl.semaphore_wait(sem, len(peers))
    def copy(self, src, dst, ss, rs, dev):
        return pltpu.make_async_remote_copy(src_ref=src, dst_ref=dst, send_sem=ss, recv_sem=rs, device_id={"dp": dev}, device_id_type=MESH)

    def pair_copy(self, b):
        s = lax.rem(b, self.ND)
        return self.copy(self.G.at[b, pl.ds(m16(self.other), self.HB)], self.D.at[s], self.ds.at[s], self.dr.at[s], self.partner)
    def phases(self):
        out = [[lambda b: self.pair_copy(b).start()], [lambda b: self.pair_copy(b).wait()]]
        per = [self.color_phases(c) for c in self.colors]
        depth = max(len(p) for p in per)
        out += [[] for _ in range(depth - 1)]
        for p in per:
            for i, f in enumerate(p):
                out[1 + i].append(f)
        return out

    def color_phases(self, c):
        G, D = self.G, self.D
        R1, O1, O1b, R2, O2, Y, SS, RS = self.bufs[c.name]
        N = self.N
        p1, p2, p3 = (self.pos[d] for d in c.dims)
        r1, l1 = self.shifted(c.dims[0], 1), self.shifted(c.dims[0], -1)
        r2, l2 = self.shifted(c.dims[1], 1), self.shifted(c.dims[1], -1)
        n1, n2, n3, h1, h2 = c.n1, c.n2, c.n3, c.h1, c.h2
        L, La, Lb, L2, La2, Lb2 = c.L, c.La, c.Lb, c.L2, c.La2, c.Lb2
        mod = lambda v, n: lax.rem(v + 4 * n, n)
        base = self.mine + c.off
        dbase = c.off
        at_ = lambda name: (lambda b: lax.rem(b, N[name]))
        sR1, sO1, sO1b, sR2, sO2, sY, sl, dsl = (at_(k) for k in ("R1", "O1", "O1b", "R2", "O2", "Y", "S", "D"))

        def ring(stage):
            if stage == 1:
                return dict(n=n1, h=h1, L=L, La=La, Lb=Lb, p=p1, right=r1, left=l1, R=R1, sR=sR1, m=c.m_rs1)
            return dict(n=n2, h=h2, L=L2, La=La2, Lb=Lb2, p=p2, right=r2, left=l2, R=R2, sR=sR2, m=c.m_rs2)
        def local(stage, b, row, k):
            if stage == 1:
                return G[b, pl.ds(m16(base + row), k), :].astype(F32) + D[dsl(b), pl.ds(m16(dbase + row), k), :].astype(F32)
            return O1[sO1(b), pl.ds(m16(row), k), :] + R1[sR1(b), pl.ds(m16(2 * (h1 - 1) * L + row), k), :].astype(F32)
        def staged(stage, b, row, k):
            if stage == 1:
                return D.at[dsl(b), pl.ds(m16(dbase + row), k)]
            return O1b.at[sO1b(b), pl.ds(m16(row), k)]
        def rs_copy(stage, b, k, direction):
            g = ring(stage)
            n, h, LL, A, Bb = g["n"], g["h"], g["L"], g["La"], g["Lb"]
            s = sl(b)
            if k < h:
                slot = mod(g["p"] + h - k + 1, n) if direction == 0 else mod(g["p"] - h + k, n)
                src = staged(stage, b, slot * LL, LL)
                dst = g["R"].at[g["sR"](b), pl.ds((k - 1) * 2 * LL + direction * LL, LL)]
            elif direction == 0:
                src = staged(stage, b, mod(g["p"] + 1, n) * LL + A, Bb)
                dst = g["R"].at[g["sR"](b), pl.ds((h - 1) * 2 * LL, Bb)]
            else:
                src = staged(stage, b, g["p"] * LL, A)
                dst = g["R"].at[g["sR"](b), pl.ds((h - 1) * 2 * LL + Bb, A)]
            m = g["m"] + 2 * (k - 1) + direction
            return self.copy(src, dst, SS.at[s, m], RS.at[s, m], g["right"] if direction == 0 else g["left"])
        def rs_step(stage, k):
            def f(b):
                g = ring(stage)
                n, h, LL, A, Bb = g["n"], g["h"], g["L"], g["La"], g["Lb"]
                s = sl(b)
                for direction in (0, 1):
                    if k > 1:
                        rs_copy(stage, b, k - 1, direction).wait()
                    slot = mod(g["p"] + h - k + 1, n) if direction == 0 else mod(g["p"] - h + k, n)
                    rin = (k - 2) * 2 * LL + direction * LL
                    def total(row, at, kk):
                        v = local(stage, b, row, kk)
                        if k > 1:
                            v = v + g["R"][g["sR"](b), pl.ds(m16(rin + at), kk), :].astype(F32)
                        return v
                    def send_part(lo, cnt):
                        def body(i, kk):
                            v = total(slot * LL + lo + i, lo + i, kk)
                            if stage == 1:
                                D[dsl(b), pl.ds(m16(dbase + slot * LL + lo + i), kk), :] = v.astype(BF16)
                            else:
                                O1b[sO1b(b), pl.ds(m16(slot * LL + lo + i), kk), :] = v.astype(BF16)
                        over_rows(cnt, body)
                    def keep_part(lo, cnt, to):
                        ref, so = (O1, sO1(b)) if stage == 1 else (O2, sO2(b))
                        def body(i, kk):
                            ref[so, pl.ds(m16(to + i), kk), :] = total(slot * LL + lo + i, lo + i, kk)
                        over_rows(cnt, body)
                    if k < h:
                        send_part(0, LL)
                        rs_copy(stage, b, k, direction).start()
                    elif direction == 0:
                        send_part(A, Bb)
                        rs_copy(stage, b, k, direction).start()
                        keep_part(0, A, Bb)
                    else:
                        send_part(0, A)
                        rs_copy(stage, b, k, direction).start()
                        keep_part(A, Bb, 0)
            return f
        def rs_end(stage):
            def f(b):
                for direction in (0, 1):
                    rs_copy(stage, b, ring(stage)["h"], direction).wait()
            return f
        def y_copy(b, k):
            s = sl(b)
            m = c.m_y + k - 1
            return self.copy(Y.at[sY(b), p3], Y.at[sY(b), p3], SS.at[s, m], RS.at[s, m], self.shifted(c.dims[2], k))
        def y_wait(b, k):
            s = sl(b)
            m = c.m_y + k - 1
            return self.copy(Y.at[sY(b), p3], Y.at[sY(b), mod(p3 - k, n3)], SS.at[s, m], RS.at[s, m], self.shifted(c.dims[2], k))
        def y_send(b):
            s = sl(b)
            def body(i, kk):
                v = O2[sO2(b), pl.ds(i, kk), :] + R2[sR2(b), pl.ds(m16(2 * (h2 - 1) * L2 + i), kk), :].astype(F32)
                Y[sY(b), p3, pl.ds(i, kk), :] = v.astype(BF16)
            over_rows(L2, body)
            for k in range(1, n3):
                y_copy(b, k).start()
        def grow(v):
            return base + mod(p1 * L + La + v, c.S)
        def y_sum(b):
            s = sl(b)
            for k in range(1, n3):
                y_wait(b, k).wait()
            def part(src, cnt, row):
                def body(i, kk):
                    v = Y[sY(b), 0, pl.ds(m16(src + i), kk), :].astype(F32)
                    for j in range(1, n3):
                        v = v + Y[sY(b), j, pl.ds(m16(src + i), kk), :].astype(F32)
                    G[b, pl.ds(m16(row + i), kk), :] = v.astype(BF16)
                over_rows(cnt, body)
            part(0, Lb2, grow(p2 * L2 + La2))
            part(Lb2, La2, grow(mod(p2 + 1, n2) * L2))
        def ag_copy(stage, b, k, direction):
            s = sl(b)
            if stage == 2:
                n, LL, A, Bb, p, right, left, m = n2, L2, La2, Lb2, p2, r2, l2, c.m_ag2
                at = lambda slot, part: grow(slot * L2) + part
            else:
                n, LL, A, Bb, p, right, left, m = n1, L, La, Lb, p1, r1, l1, c.m_ag1
                at = lambda slot, part: base + slot * L + part
            if k == 1:
                row, cnt = (at(mod(p + 1, n), 0), A) if direction == 0 else (at(p, A), Bb)
            else:
                row, cnt = (at(mod(p - (k - 2), n), 0) if direction == 0 else at(mod(p + 1 + (k - 2), n), 0)), LL
            ref = G.at[b, pl.ds(m16(row), cnt)]
            mm = m + 2 * (k - 1) + direction
            return self.copy(ref, ref, SS.at[s, mm], RS.at[s, mm], right if direction == 0 else left)
        def ag_in(stage, b, k, direction):
            s = sl(b)
            if stage == 2:
                n, LL, A, Bb, p, right, left, m = n2, L2, La2, Lb2, p2, r2, l2, c.m_ag2
                at = lambda slot, part: grow(slot * L2) + part
            else:
                n, LL, A, Bb, p, right, left, m = n1, L, La, Lb, p1, r1, l1, c.m_ag1
                at = lambda slot, part: base + slot * L + part
            if k == 1:
                row, cnt = (at(p, 0), A) if direction == 0 else (at(mod(p + 1, n), A), Bb)
            else:
                row, cnt = (at(mod(p - 1 - (k - 2), n), 0) if direction == 0 else at(mod(p + 2 + (k - 2), n), 0)), LL
            ref = G.at[b, pl.ds(m16(row), cnt)]
            mm = m + 2 * (k - 1) + direction
            return self.copy(ref, ref, SS.at[s, mm], RS.at[s, mm], right if direction == 0 else left)
        def ag_wait(stage, b, k):
            for direction in (0, 1):
                ag_copy(stage, b, k, direction).wait_send()
                ag_in(stage, b, k, direction).wait_recv()
        def ag_start(stage, b, k):
            for direction in (0, 1):
                ag_copy(stage, b, k, direction).start()
        def pair(b):
            s = sl(b)
            ref = G.at[b, pl.ds(m16(base), c.S)]
            return self.copy(ref, ref, SS.at[s, c.m_pair], RS.at[s, c.m_pair], self.partner)
        def pair_in(b):
            s = sl(b)
            ref = G.at[b, pl.ds(m16(self.other + c.off), c.S)]
            return self.copy(ref, ref, SS.at[s, c.m_pair], RS.at[s, c.m_pair], self.partner)

        out = []
        for k in range(1, h1 + 1):
            out.append(rs_step(1, k))
        for k in range(1, h2 + 1):
            if k == 1:
                out.append(lambda b: (rs_end(1)(b), rs_step(2, 1)(b)))
            else:
                out.append(rs_step(2, k))
        out.append(lambda b: (rs_end(2)(b), y_send(b)))
        out.append(lambda b: (y_sum(b), ag_start(2, b, 1)))
        for k in range(2, h2 + 1):
            out.append(lambda b, k=k: (ag_wait(2, b, k - 1), ag_start(2, b, k)))
        out.append(lambda b: (ag_wait(2, b, h2), ag_start(1, b, 1)))
        for k in range(2, h1 + 1):
            out.append(lambda b, k=k: (ag_wait(1, b, k - 1), ag_start(1, b, k)))
        out.append(lambda b: (ag_wait(1, b, h1), pair(b).start()))
        out.append(lambda b: (pair(b).wait_send(), pair_in(b).wait_recv()))
        return out


TOK, DIM, FF = 1024, 768, 3072
TF = 256
NT = FF // TF
PARTS = 6
K = NT // PARTS
HALF = 512

def dot(a, b):
    return jnp.dot(a, b, preferred_element_type=F32)
def dot_nt(a, b):
    return lax.dot_general(a, b, (((1,), (1,)), ((), ())), preferred_element_type=F32)

OFFS = {
    "A": [0, 1, 4, 5, 6, 7, 8, 9, 10, 11, 12, 13, 14, 15, 18, 19],
    "B": [0, 1, 3, 4, 5, 6, 7, 8, 9, 10, 11, 12, 13, 14, 16, 17],
    "C": [0, 1, 2, 3, 5, 7, 8, 9, 10, 11, 12, 13, 14, 15, 17, 18],
}
SLOTS = {"R1": 4, "O1": 2, "O1b": 2, "R2": 3, "O2": 2, "Y": 2, "D": 5, "S": 12}

def mega(comm, x_hbm, dy_hbm, wg_hbm, wu_hbm, wd_hbm, G, A, AT, DY, DYT, H, ACC, TH, TG, TU, WG, WU, WD, wsem, xsem, *cs):
    B = comm.B
    comm.setup(G, cs)
    def wcopies(u):
        q = lax.div(u, NT)
        layer = lax.rem(q, 2)
        j = lax.rem(u, NT)
        s = lax.rem(u, 2)
        f = pl.multiple_of(j * TF, TF)
        return (pltpu.make_async_copy(wg_hbm.at[layer, :, pl.ds(f, TF)], WG.at[s], wsem.at[s, 0]),
                pltpu.make_async_copy(wu_hbm.at[layer, :, pl.ds(f, TF)], WU.at[s], wsem.at[s, 1]),
                pltpu.make_async_copy(wd_hbm.at[layer, pl.ds(f, TF), :], WD.at[s], wsem.at[s, 2]))
    def wstart(u):
        for c in wcopies(u):
            c.start()
    def wwait(u):
        for c in wcopies(u):
            c.wait()
    xin = pltpu.make_async_copy(x_hbm, H, xsem.at[0])
    xagain = pltpu.make_async_copy(x_hbm, A, xsem.at[0])
    dyin = pltpu.make_async_copy(dy_hbm, DY, xsem.at[1])
    xin.start(); dyin.start(); wstart(0)
    comm.barrier()

    def rows_of(i, n):
        return pl.ds(pl.multiple_of(i * n, n), n)
    def each(n, body):
        def step(i, _):
            body(rows_of(i, n))
            return 0
        lax.fori_loop(0, TOK // n, step, 0)
    def norm(src, r):
        wide = src[r, :].astype(F32)
        scale = lax.rsqrt(jnp.mean(wide * wide, -1, keepdims=True) + 1e-6)
        return (wide * scale).astype(BF16)
    def zero(r):
        ACC[r, :] = jnp.zeros((r.size, DIM), F32)

    xin.wait()
    def first(r):
        A[r, :] = norm(H, r)
        zero(r)
    each(128, first)

    def forward(u, _):
        s = lax.rem(u, 2)
        wwait(u)
        wstart(u + 1)
        def half(r):
            a = A[r, :]
            gate = dot(a, WG[s])
            up = dot(a, WU[s])
            hid = (gate * jax.nn.sigmoid(gate) * up).astype(BF16)
            ACC[r, :] += dot(hid, WD[s])
        for i in range(TOK // HALF):
            half(pl.ds(i * HALF, HALF))
        return 0
    lax.fori_loop(0, NT, forward, 0)
    dyin.wait()
    def between(r):
        H[r, :] = (H[r, :].astype(F32) + ACC[r, :].astype(BF16).astype(F32)).astype(BF16)
        a = norm(H, r)
        A[r, :] = a
        AT[:, r] = a.T
        DYT[:, r] = DY[r, :].T
        zero(r)
    each(128, between)

    def backward(u, t, want_input):
        s = lax.rem(u, 2)
        b = lax.div(t, K)
        jt = lax.rem(t, K)
        wwait(u)
        @pl.when(u + 1 < 3 * NT)
        def _():
            wstart(u + 1)
        for i in range(TOK // HALF):
            r = pl.ds(i * HALF, HALF)
            a = A[r, :]
            gate = dot(a, WG[s])
            up = dot(a, WU[s])
            dh = dot_nt(DY[r, :], WD[s]).astype(BF16).astype(F32)
            sig = jax.nn.sigmoid(gate)
            act = gate * sig
            TH[r, :] = (act * up).astype(BF16)
            du = (dh * act).astype(BF16)
            dg = (dh * up * (sig * (1.0 + gate * (1.0 - sig)))).astype(BF16)
            TU[r, :] = du
            TG[r, :] = dg
            if want_input:
                ACC[r, :] += dot_nt(dg, WG[s]) + dot_nt(du, WU[s])
        for mat, (lhs, rhs) in enumerate(((AT, TG), (AT, TU), (DYT, TH))):
            d = dot(lhs[...], rhs[...]).astype(BF16)
            for k in range(TF // LANES):
                row = (mat * (K * TF // LANES) + jt * (TF // LANES) + k) * DIM
                G[b, pl.ds(m16(row), DIM), :] = d[:, k * LANES:(k + 1) * LANES]

    def middle():
        xagain.start()
        def body(r):
            da = ACC[r, :].astype(BF16).astype(F32)
            wide = H[r, :].astype(F32)
            scale = lax.rsqrt(jnp.mean(wide * wide, -1, keepdims=True) + 1e-6)
            ds = jnp.sum(da * wide, -1, keepdims=True)
            dwide = da * scale - wide * (ds * scale * scale * scale * (1.0 / DIM))
            d = (DY[r, :].astype(F32) + dwide.astype(BF16).astype(F32)).astype(BF16)
            DY[r, :] = d
            DYT[:, r] = d.T
        each(128, body)
        xagain.wait()
        def again(r):
            a = norm(A, r)
            A[r, :] = a
            AT[:, r] = a.T
        each(128, again)

    phases = comm.phases()
    events = []
    for ph, fns in enumerate(phases):
        if ph == 0:
            events += [(0, f) for f in fns]
        else:
            cols = [c.name for c in comm.colors]
            fs = list(fns)
            if ph == 1:
                events.append((1, fs.pop(0)))
            for name, f in zip(cols, fs):
                events.append((OFFS[name][ph], f))
    last = max(o for o, _ in events)
    depth = last // K + 1
    def tick(t):
        it = lax.div(t, K) - 1
        for sub in range(K):
            if not any(o % K == sub for o, _ in events):
                continue
            @pl.when(lax.rem(t, K) == sub)
            def _():
                for i in reversed(range(depth)):
                    fs = [f for o, f in events if o == sub + K * i]
                    if not fs:
                        continue
                    b = it - i
                    @pl.when((b >= 0) & (b < B))
                    def _():
                        for f in fs:
                            f(b)
    def step(t, _):
        tick(t)
        @pl.when(t < NT)
        def _():
            backward(t + NT, t, True)
        @pl.when(t == NT)
        def _():
            middle()
        @pl.when((t >= NT) & (t < 2 * NT))
        def _():
            backward(t + NT, t, False)
        return 0
    lax.fori_loop(0, K * B + last + 1, step, 0)

def gradients(comm, x, dy, wg, wu, wd, vmem=37_000_000):
    V = pltpu.VMEM
    scratch = [V((TOK, DIM), BF16), V((DIM, TOK), BF16), V((TOK, DIM), BF16), V((DIM, TOK), BF16), V((TOK, DIM), BF16), V((TOK, DIM), F32),
               V((TOK, TF), BF16), V((TOK, TF), BF16), V((TOK, TF), BF16),
               V((2, DIM, TF), BF16), V((2, DIM, TF), BF16), V((2, TF, DIM), BF16),
               pltpu.SemaphoreType.DMA((2, 3)), pltpu.SemaphoreType.DMA((2,))]
    return pl.pallas_call(
        functools.partial(mega, comm),
        out_shape=pltpu.VMEM((comm.B, comm.TB, LANES), BF16),
        in_specs=[pl.BlockSpec(memory_space=pl.ANY)] * 5, out_specs=pl.BlockSpec(memory_space=pltpu.VMEM),
        scratch_shapes=scratch + comm.scratch(),
        compiler_params=pltpu.CompilerParams(collective_id=0, has_side_effects=True, vmem_limit_bytes=vmem),
    )(x, dy, wg, wu, wd)

def adam_all(weights, m, v, g, parts, rows=256, nbuf=4, nout=2, ahead=3, layers=2):
    dim, ff = weights[0].shape[1:]
    blocks = dim // LANES
    per = ff // parts // LANES
    down_tiles = ff // rows
    across = ff // dim
    S = layers * down_tiles
    def body(wg, wu, wd, mg, mu, md, vg, vu, vd, gr, owg, owu, owd, omg, omu, omd, ovg, ovu, ovd, wb, mb, vb, xw, xm, xv, isem, osem):
        ins_, outs_ = ((wg, mg, vg), (wu, mu, vu), (wd, md, vd)), ((owg, omg, ovg), (owu, omu, ovu), (owd, omd, ovd))
        def place(which, i):
            l, j = lax.div(i, down_tiles), lax.rem(i, down_tiles)
            if which == 2:
                return l, j * rows, 0
            return l, lax.div(j, across) * rows, lax.rem(j, across) * dim
        def at(which, i):
            l, r, c = place(which, i)
            return (l, pl.ds(pl.multiple_of(r, rows), rows), pl.ds(pl.multiple_of(c, dim), dim))
        def load(which, i):
            s = lax.rem(i + which * S, nbuf)
            return [pltpu.make_async_copy(ins_[which][k].at[at(which, i)], b.at[s], isem.at[s, k]) for k, b in enumerate((wb, mb, vb))]
        def store(which, i):
            s = lax.rem(i + which * S, nout)
            return [pltpu.make_async_copy(b.at[s], outs_[which][k].at[at(which, i)], osem.at[s, k]) for k, b in enumerate((xw, xm, xv))]
        def start(cs):
            for x in cs:
                x.start()
        def wait(cs):
            for x in cs:
                x.wait()
        def compute(which, i):
            l, r, c = place(which, i)
            s, so = lax.rem(i + which * S, nbuf), lax.rem(i + which * S, nout)
            def one(gv, where):
                mm = 0.9 * mb[(s, *where)] + 0.1 * gv
                vv = 0.95 * vb[(s, *where)] + 0.05 * gv * gv
                ww = wb[(s, *where)].astype(F32)
                step = mm * lax.rsqrt(vv + 1e-8) + 0.1 * ww
                xw[(so, *where)] = (ww - 0.02 * step).astype(BF16)
                xm[(so, *where)] = mm
                xv[(so, *where)] = vv
            first = (layers - 1 - l) * parts
            if which < 2:
                for k in range(blocks):
                    col = lax.div(c, LANES) + k
                    b = first + lax.div(col, per)
                    row = (which * per + lax.rem(col, per)) * dim + r
                    one(gr[b, pl.ds(pl.multiple_of(row, rows), rows), :].astype(F32), (slice(None), pl.ds(k * LANES, LANES)))
            else:
                for k in range(rows // LANES):
                    col = lax.div(r, LANES) + k
                    b = first + lax.div(col, per)
                    for q in range(0, dim, 256):
                        row = (which * per + lax.rem(col, per)) * dim + q
                        one(gr[b, pl.ds(pl.multiple_of(row, 256), 256), :].astype(F32).T, (pl.ds(k * LANES, LANES), pl.ds(q, 256)))
        def each(i, f):
            for which in range(3):
                @pl.when((i >= which * S) & (i < (which + 1) * S))
                def _():
                    f(which, i - which * S)
        for i in range(ahead):
            start(load(0, i))
        def step(i, _):
            each(i + ahead, lambda w, t: start(load(w, t)))
            each(i, lambda w, t: wait(load(w, t)))
            each(i - nout, lambda w, t: wait(store(w, t)))
            each(i, lambda w, t: (compute(w, t), start(store(w, t))))
            return 0
        lax.fori_loop(0, 3 * S, step, 0)
        for i in range(S - nout, S):
            wait(store(2, i))
    V, D = pltpu.VMEM, pltpu.SemaphoreType.DMA
    t = (rows, dim)
    anys = pl.BlockSpec(memory_space=pl.ANY)
    out = pl.pallas_call(
        body,
        out_shape=[jax.ShapeDtypeStruct(x.shape, x.dtype) for x in (*weights, *m, *v)],
        in_specs=[anys] * 9 + [pl.BlockSpec(memory_space=pltpu.VMEM)],
        out_specs=[anys] * 9,
        scratch_shapes=[V((nbuf, *t), BF16), V((nbuf, *t), F32), V((nbuf, *t), F32), V((nout, *t), BF16), V((nout, *t), F32), V((nout, *t), F32), D((nbuf, 3)), D((nout, 3))],
        compiler_params=pltpu.CompilerParams(vmem_limit_bytes=32_000_000),
    )(*weights, *m, *v, pltpu.with_memory_space_constraint(g, pltpu.VMEM))
    return tuple(out)
TILE = 16
COLORS = (("A", 96 * TILE, "xzy"), ("B", 128 * TILE, "yzx"), ("C", 64 * TILE, "zxy"))
SIZES = {"x": 4, "y": 4, "z": 8}
def make_comm():
    return Comm(SIZES, COLORS, 2 * PARTS, SLOTS)

def train_step(comm, x, dy, *arrays):
    weights, m, v = (arrays[i:i + 3] for i in (0, 3, 6))
    g = gradients(comm, x[0], dy[0], *weights)
    return adam_all(weights, m, v, g, PARTS, rows=128, nbuf=8, nout=4, ahead=7)


def solution(mesh):
    comm = make_comm()
    return jax.shard_map(
        functools.partial(train_step, comm),
        mesh=mesh,
        in_specs=(P(("rep", "dp"), None, None),) * 2 + (P(None, None, None),) * 9,
        out_specs=(P("rep", None, None),) * 9,
        check_vma=False,
    )
```
